16 devices in a mesh: rep: 2 (over y, z), dp: 8 (over x, core).
Axes of the slice: x: 4, y: 2, z: 1, core: 2. Of those that a mesh axis runs over, the one named last changes fastest.
The devices are a block of a 4x4x8 slice.
Arguments:
- x: bfloat16 [16, 2048, 768], P(('rep', 'dp')), parts along dimension 0
- dy: bfloat16 [16, 2048, 768], P(('rep', 'dp')), parts along dimension 0
- w_gate: bfloat16 [2, 768, 2304], replicated
- w_up: bfloat16 [2, 768, 2304], replicated
- w_down: bfloat16 [2, 2304, 768], replicated
- m_w_gate: float32 [2, 768, 2304], replicated
- m_w_up: float32 [2, 768, 2304], replicated
- m_w_down: float32 [2, 2304, 768], replicated
- v_w_gate: float32 [2, 768, 2304], replicated
- v_w_up: float32 [2, 768, 2304], replicated
- v_w_down: float32 [2, 2304, 768], replicated
Outputs:
- output 1: bfloat16 [4, 768, 2304], P('rep'), parts along dimension 0
- output 2: bfloat16 [4, 768, 2304], P('rep'), parts along dimension 0
- output 3: bfloat16 [4, 2304, 768], P('rep'), parts along dimension 0
- output 4: float32 [4, 768, 2304], P('rep'), parts along dimension 0
- output 5: float32 [4, 768, 2304], P('rep'), parts along dimension 0
- output 6: float32 [4, 2304, 768], P('rep'), parts along dimension 0
- output 7: float32 [4, 768, 2304], P('rep'), parts along dimension 0
- output 8: float32 [4, 768, 2304], P('rep'), parts along dimension 0
- output 9: float32 [4, 2304, 768], P('rep'), parts along dimension 0
There are 2 independent parts. The reference program is written for one: setup_inputs(seed, part) draws one part's arguments, and reference() takes and returns one part's arrays. A program takes and returns all parts, laid end to end along the dimension named above; an argument that names none is the same for every part.
All inputs are finite; a program needn't handle non-finite values.
Results may differ from the reference program's by a relative error of at most 0.022.
Values are sent between devices in bfloat16 or wider.
A program may use at most 768 MiB of HBM per device.

```python
import jax
import jax.numpy as jnp
from jax import lax

SEQUENCES = 8
TOKENS = 2048
D = 768
FF = 2304
LAYERS = 2
NAMES = ("w_gate", "w_up", "w_down")
SHAPES = {"w_gate": (LAYERS, D, FF), "w_up": (LAYERS, D, FF), "w_down": (LAYERS, FF, D)}


def bump(key, n, height):
    away = (jnp.arange(n, dtype=jnp.int32) - jax.random.randint(key, (), 0, n, jnp.int32)) % n
    return jnp.where(away < n // 8, height, 1.0)


def together(key, own, strength):
    shared = jax.random.normal(key, own.shape[1:], jnp.float32)
    return (own + strength * shared) * lax.rsqrt(1 + strength * strength)


def setup_inputs(seed: int = 0, part: int = 0) -> dict:
    kx, kdy, ka, kb, kz, kf, kh, kl, *keys = jax.random.split(jax.random.key(seed), 8 + 3 * len(NAMES))
    kx, kdy, ka, kb = (jax.random.fold_in(k, part) for k in (kx, kdy, ka, kb))
    kw, km, kv = (keys[i::3] for i in range(3))
    shape = (SEQUENCES, TOKENS, D)
    much_x, much_dy = jax.random.uniform(kz, (2,), jnp.float32, 0.0, 1.0)
    loud = 2.0 ** jax.random.uniform(jax.random.fold_in(kz, 1), (), jnp.float32, -1.0, 2.0)
    layers = 2.0 ** jax.random.uniform(kl, (LAYERS, 1, 1), jnp.float32, -1.0, 1.0)
    x = together(ka, jax.random.normal(kx, shape, jnp.float32), much_x) * bump(kf, D, 4.0)
    dy = together(kb, jax.random.normal(kdy, shape, jnp.float32), much_dy)
    drawn = {"x": x.astype(jnp.bfloat16), "dy": (loud * dy * (SEQUENCES * TOKENS) ** -0.5).astype(jnp.bfloat16)}
    for key, name in zip(kw, NAMES, strict=True):
        w = jax.random.normal(key, SHAPES[name], jnp.float32) * SHAPES[name][1] ** -0.5
        drawn[name] = (w * {"w_gate": 1.0, "w_up": bump(kh, FF, 4.0), "w_down": layers}[name]).astype(jnp.bfloat16)
    for key, name in zip(km, NAMES, strict=True):
        drawn[f"m_{name}"] = 0.1 * jax.random.normal(key, SHAPES[name], jnp.float32)
    for key, name in zip(kv, NAMES, strict=True):
        drawn[f"v_{name}"] = jax.random.uniform(key, SHAPES[name], jnp.float32, 0.005, 0.015)
    return drawn


def matmul(a, w):
    return jnp.dot(a, w, preferred_element_type=jnp.float32).astype(jnp.bfloat16)


def normed(h):
    wide = h.astype(jnp.float32)
    scale = lax.rsqrt(jnp.mean(wide**2, -1, keepdims=True) + 1e-6)
    return (wide * scale).astype(jnp.bfloat16)


def layer(h, w):
    a = normed(h)
    gate = jnp.dot(a, w["w_gate"], preferred_element_type=jnp.float32)
    up = jnp.dot(a, w["w_up"], preferred_element_type=jnp.float32)
    return h + matmul((jax.nn.silu(gate) * up).astype(jnp.bfloat16), w["w_down"])


def adamw(w, m, v, g):
    m = 0.9 * m + 0.1 * g
    v = 0.95 * v + 0.05 * g * g
    step = m * lax.rsqrt(v + 1e-8) + 0.1 * w
    return (w - 0.02 * step).astype(jnp.bfloat16), m, v


def clipped(gradients, sum_of_squares, count):
    factor = jnp.minimum(1.0, 0.5 * lax.rsqrt(sum_of_squares / count + 1e-30))
    return [g * factor for g in gradients]


def stack(weights, h):
    return lax.scan(lambda h, w: (layer(h, w), None), h, weights)[0]


def reference(x, dy, w_gate, w_up, w_down, m_w_gate, m_w_up, m_w_down, v_w_gate, v_w_up, v_w_down):
    weights = dict(zip(NAMES, (w_gate, w_up, w_down), strict=True))

    def take(so_far, sequence):
        h, by_y = sequence
        _, back = jax.vjp(lambda w: stack(w, h), weights)
        return jax.tree.map(lambda total, term: total + term.astype(jnp.float32), so_far, back(by_y)[0]), None

    none_yet = {name: jnp.zeros(w.shape, jnp.float32) for name, w in weights.items()}
    by_weights, _ = lax.scan(take, none_yet, (x, dy))
    gradients = [by_weights[name].astype(jnp.bfloat16).astype(jnp.float32) for name in NAMES]
    gradients = clipped(gradients, sum(jnp.sum(g * g) for g in gradients), sum(g.size for g in gradients))
    new = [
        adamw(w.astype(jnp.float32), m, v, g)
        for w, m, v, g in zip((w_gate, w_up, w_down), (m_w_gate, m_w_up, m_w_down), (v_w_gate, v_w_up, v_w_down), gradients, strict=True)
    ]
    return tuple(one[which] for which in range(3) for one in new)
```

```python
import functools

import jax
import jax.numpy as jnp
from jax import lax
from jax.experimental import pallas as pl
from jax.experimental.pallas import tpu as pltpu
from jax.sharding import PartitionSpec as P

F32, BF16 = jnp.float32, jnp.bfloat16
WIDTH = 256
CHUNK = 512
VMEM_LIMIT = 60 * 1024 * 1024
NT = (((1,), (1,)), ((), ()))


def dot(a, b):
    return jnp.dot(a, b, preferred_element_type=F32)


def dot_nt(a, b):
    return lax.dot_general(a, b, NT, preferred_element_type=F32)


def normed(h):
    wide = h.astype(F32)
    scale = lax.rsqrt(jnp.mean(wide**2, -1, keepdims=True) + 1e-6)
    return (wide * scale).astype(BF16)


def forward_kernel(a_ref, h_ref, wg_ref, wu_ref, wd_ref, out_ref, acc):
    s = pl.program_id(0)
    tokens = a_ref.shape[0]

    @pl.when(s == 0)
    def _():
        acc[...] = jnp.zeros_like(acc)

    def body(t, _):
        rows = pl.ds(pl.multiple_of(t * CHUNK, CHUNK), CHUNK)
        a = a_ref[rows, :]
        gate = dot(a, wg_ref[0])
        up = dot(a, wu_ref[0])
        act = (gate * jax.nn.sigmoid(gate) * up).astype(BF16)
        acc[rows, :] += dot(act, wd_ref[0])
        return 0

    lax.fori_loop(0, tokens // CHUNK, body, 0)

    @pl.when(s == pl.num_programs(0) - 1)
    def _():
        out_ref[...] = h_ref[...] + acc[...].astype(BF16)


def forward(layer, a, h, wg, wu, wd):
    tokens, d = a.shape
    ff = wg.shape[-1]
    whole = pl.BlockSpec((tokens, d), lambda s: (0, 0))
    return pl.pallas_call(
        forward_kernel,
        grid=(ff // WIDTH,),
        in_specs=[
            whole,
            whole,
            pl.BlockSpec((1, d, WIDTH), lambda s: (layer, 0, s)),
            pl.BlockSpec((1, d, WIDTH), lambda s: (layer, 0, s)),
            pl.BlockSpec((1, WIDTH, d), lambda s: (layer, s, 0)),
        ],
        out_specs=whole,
        out_shape=jax.ShapeDtypeStruct((tokens, d), BF16),
        scratch_shapes=[pltpu.VMEM((tokens, d), F32)],
        compiler_params=pltpu.CompilerParams(vmem_limit_bytes=VMEM_LIMIT, dimension_semantics=("arbitrary",)),
        name="forward",
    )(a, h, wg, wu, wd)


def backward_kernel(with_da, a_ref, at_ref, dy_ref, dyt_ref, wg_ref, wu_ref, wd_ref, g_ref, da_ref, gu_buf, act_buf, acc):
    s = pl.program_id(0)
    tokens, d = a_ref.shape

    if with_da:

        @pl.when(s == 0)
        def _():
            acc[...] = jnp.zeros_like(acc)

    def body(t, _):
        rows = pl.ds(pl.multiple_of(t * CHUNK, CHUNK), CHUNK)
        a = a_ref[rows, :]
        gate = dot(a, wg_ref[0])
        up = dot(a, wu_ref[0])
        dact = dot_nt(dy_ref[rows, :], wd_ref[0]).astype(BF16).astype(F32)
        sig = jax.nn.sigmoid(gate)
        silu = gate * sig
        act_buf[rows, :] = (silu * up).astype(BF16)
        dup = (dact * silu).astype(BF16)
        dgate = (dact * up * (sig + silu * (1 - sig))).astype(BF16)
        gu_buf[rows, :WIDTH] = dgate
        gu_buf[rows, WIDTH:] = dup
        if with_da:
            acc[rows, :] += dot_nt(dgate, wg_ref[0]) + dot_nt(dup, wu_ref[0])
        return 0

    lax.fori_loop(0, tokens // CHUNK, body, 0)

    def weights(i, _):
        rows = pl.ds(pl.multiple_of(i * 256, 256), 256)
        both = dot(at_ref[rows, :], gu_buf[...]).astype(BF16)
        g_ref[0, pl.ds(pl.multiple_of(i * 256, 256), 256), :] = both[:, :WIDTH]
        g_ref[0, pl.ds(pl.multiple_of(d + i * 256, 256), 256), :] = both[:, WIDTH:]
        g_ref[0, pl.ds(pl.multiple_of(2 * d + i * 256, 256), 256), :] = dot(dyt_ref[rows, :], act_buf[...]).astype(BF16)
        return 0

    lax.fori_loop(0, d // 256, weights, 0)

    if with_da:

        @pl.when(s == pl.num_programs(0) - 1)
        def _():
            da_ref[...] = acc[...].astype(BF16)


def backward(layer, with_da, a, dy, wg, wu, wd):
    tokens, d = a.shape
    ff = wg.shape[-1]
    whole = pl.BlockSpec((tokens, d), lambda s: (0, 0))
    wholet = pl.BlockSpec((d, tokens), lambda s: (0, 0))
    da_rows = tokens if with_da else 8
    return pl.pallas_call(
        functools.partial(backward_kernel, with_da),
        grid=(ff // WIDTH,),
        in_specs=[
            whole,
            wholet,
            whole,
            wholet,
            pl.BlockSpec((1, d, WIDTH), lambda s: (layer, 0, s)),
            pl.BlockSpec((1, d, WIDTH), lambda s: (layer, 0, s)),
            pl.BlockSpec((1, WIDTH, d), lambda s: (layer, s, 0)),
        ],
        out_specs=[
            pl.BlockSpec((1, 3 * d, WIDTH), lambda s: (s, 0, 0)),
            pl.BlockSpec((da_rows, d), lambda s: (0, 0)),
        ],
        out_shape=[
            jax.ShapeDtypeStruct((ff // WIDTH, 3 * d, WIDTH), BF16),
            jax.ShapeDtypeStruct((da_rows, d), BF16),
        ],
        scratch_shapes=[
            pltpu.VMEM((tokens, 2 * WIDTH), BF16),
            pltpu.VMEM((tokens, WIDTH), BF16),
            pltpu.VMEM((da_rows, d), F32),
        ],
        compiler_params=pltpu.CompilerParams(vmem_limit_bytes=VMEM_LIMIT, dimension_semantics=("arbitrary",)),
        name="backward",
    )(a, a.T, dy, dy.T, wg, wu, wd)


def norm_backward(h, da, dh):
    _, back = jax.vjp(normed, h)
    return dh + back(da)[0]


def adamw_kernel(f_ref, g0_ref, g1_ref, *refs):
    ws, ms, vs = refs[0:3], refs[3:6], refs[6:9]
    new_ws, new_ms, new_vs = refs[9:12], refs[12:15], refs[15:18]
    factor = f_ref[0]
    d = ws[0].shape[1]
    layer = pl.program_id(0)

    def update(g, w, m, v, new_w, new_m, new_v, rows, columns):
        at = (0, rows, columns)
        g = g.astype(F32) * factor
        m = 0.9 * m[at] + 0.1 * g
        v = 0.95 * v[at] + 0.05 * g * g
        new_m[at] = m
        new_v[at] = v
        wide = w[at].astype(F32)
        new_w[at] = (wide - 0.02 * (m * lax.rsqrt(v + 1e-8) + 0.1 * wide)).astype(BF16)

    def take(g_ref):
        for i in range(2):
            for j in range(d // 256):
                rows = slice(j * 256, (j + 1) * 256)
                update(g_ref[0, i * d + j * 256 : i * d + (j + 1) * 256, :], *(r[i] for r in (ws, ms, vs, new_ws, new_ms, new_vs)), rows, slice(None))
        for j in range(d // 256):
            g = g_ref[0, 2 * d + j * 256 : 2 * d + (j + 1) * 256, :].astype(F32).T
            update(g, *(r[2] for r in (ws, ms, vs, new_ws, new_ms, new_vs)), slice(None), slice(j * 256, (j + 1) * 256))

    @pl.when(layer == 0)
    def _():
        take(g0_ref)

    @pl.when(layer != 0)
    def _():
        take(g1_ref)


def adamw(factor, g, weights, m, v):
    layers, d, ff = weights[0].shape
    n = ff // WIDTH
    wide = pl.BlockSpec((1, d, WIDTH), lambda l, s: (l, 0, s))
    tall = pl.BlockSpec((1, WIDTH, d), lambda l, s: (l, s, 0))
    three = [wide, wide, tall]
    return pl.pallas_call(
        adamw_kernel,
        grid=(layers, n),
        in_specs=[
            pl.BlockSpec(memory_space=pltpu.SMEM),
            pl.BlockSpec((1, 3 * d, WIDTH), lambda l, s: (jnp.where(l == 0, s, n - 1), 0, 0)),
            pl.BlockSpec((1, 3 * d, WIDTH), lambda l, s: (jnp.where(l == 0, 0, s), 0, 0)),
        ]
        + three * 3,
        out_specs=three * 3,
        out_shape=[jax.ShapeDtypeStruct(w.shape, t) for t in (BF16, F32, F32) for w in weights],
        compiler_params=pltpu.CompilerParams(vmem_limit_bytes=VMEM_LIMIT, dimension_semantics=("arbitrary", "arbitrary")),
        name="adamw",
    )(factor, *g, *weights, *m, *v)


def solution(mesh):
    def step(x, dy, *arrays):
        weights, m, v = (arrays[i : i + 3] for i in (0, 3, 6))
        layers = weights[0].shape[0]
        h, kept = x[0], []
        for number in range(layers):
            a = normed(h)
            kept.append((h, a))
            if number < layers - 1:
                h = forward(number, a, h, *weights)
        by_h, g = dy[0], [None] * layers
        for number in reversed(range(layers)):
            h, a = kept[number]
            part, da = backward(number, number > 0, a, by_h, *weights)
            g[number] = lax.psum(part, "dp")
            if number > 0:
                by_h = norm_backward(h, da, by_h)
        squares = sum(jnp.sum(one.astype(F32) ** 2) for one in g)
        count = sum(one.size for one in g)
        factor = jnp.minimum(1.0, 0.5 * lax.rsqrt(squares / count + 1e-30))
        return tuple(adamw(factor.reshape(1), g, weights, m, v))

    return jax.shard_map(
        step,
        mesh=mesh,
        in_specs=(P(("rep", "dp"), None, None),) * 2 + (P(None, None, None),) * 9,
        out_specs=(P("rep", None, None),) * 9,
        check_vma=False,
    )
```

```python
import functools

import jax
import jax.numpy as jnp
from jax import lax
from jax.experimental import pallas as pl
from jax.experimental.pallas import tpu as pltpu
from jax.sharding import PartitionSpec as P

F32, BF16 = jnp.float32, jnp.bfloat16
MESH = pl.DeviceIdType.MESH
WIDTH = 768
STRIP = 256
CHUNK = 512
ROWS = 256
VMEM_LIMIT = 63 * 1024 * 1024
NT = (((1,), (1,)), ((), ()))


def dot(a, b):
    return jnp.dot(a, b, preferred_element_type=F32)


def dot_nt(a, b):
    return lax.dot_general(a, b, NT, preferred_element_type=F32)


def norm_scale(wide):
    return lax.rsqrt(jnp.mean(wide**2, -1, keepdims=True) + 1e-6)


def normed(h):
    wide = h.astype(F32)
    return (wide * norm_scale(wide)).astype(BF16)


def once(shape):
    return pl.BlockSpec(shape, lambda *_: (0,) * len(shape), pipeline_mode=pl.Buffered(1))


def forward_kernel(h_ref, wg_ref, wu_ref, wd_ref, out_ref, a_buf, acc):
    s = pl.program_id(0)
    tokens = a_buf.shape[0]
    chunks = [pl.ds(t, CHUNK) for t in range(0, tokens, CHUNK)]

    @pl.when(s == 0)
    def _():
        for rows in chunks:
            a_buf[rows, :] = normed(h_ref[0, rows, :])
            acc[rows, :] = jnp.zeros((CHUNK, acc.shape[1]), F32)

    for rows in chunks:
        a = a_buf[rows, :]
        gate = dot(a, wg_ref[0])
        up = dot(a, wu_ref[0])
        act = (gate * jax.nn.sigmoid(gate) * up).astype(BF16)
        acc[rows, :] += dot(act, wd_ref[0])

    @pl.when(s == pl.num_programs(0) - 1)
    def _():
        for rows in chunks:
            out_ref[0, rows, :] = h_ref[0, rows, :] + acc[rows, :].astype(BF16)


def weight_specs(layer, d):
    wide = pl.BlockSpec((1, d, WIDTH), lambda s: (layer, 0, s))
    return [wide, wide, pl.BlockSpec((1, WIDTH, d), lambda s: (layer, s, 0))]


def forward(layer, h, weights):
    _, tokens, d = h.shape
    ff = weights[0].shape[-1]
    return pl.pallas_call(
        forward_kernel,
        grid=(ff // WIDTH,),
        in_specs=[once(h.shape)] + weight_specs(layer, d),
        out_specs=once(h.shape),
        out_shape=jax.ShapeDtypeStruct(h.shape, BF16),
        scratch_shapes=[pltpu.VMEM((tokens, d), BF16), pltpu.VMEM((tokens, d), F32)],
        compiler_params=pltpu.CompilerParams(vmem_limit_bytes=VMEM_LIMIT, dimension_semantics=("arbitrary",)),
        name="forward",
    )(h, *weights)


class Exchange:
    def __init__(self, n, g_buf, got_half, got_far, got_near, own_ref, squares, sems):
        self.g_buf, self.got_half, self.got_far, self.got_near = g_buf, got_half, got_far, got_near
        self.own_ref, self.squares = own_ref, squares
        self.swap_sems, self.sems = sems
        me = lax.axis_index("dp")
        self.core, self.chip = lax.rem(me, 2), me // 2
        self.chips = n // 2
        self.right = lax.rem(self.chip + 1, self.chips)
        self.left = lax.rem(self.chip + self.chips - 1, self.chips)
        self.far = lax.rem(self.chip + 2, self.chips)
        self.share = got_near.shape[2]

    def to(self, chip, core):
        return {"dp": chip * 2 + core}

    def barrier(self):
        barrier = pltpu.get_barrier_semaphore()
        peers = [(self.chip, 1 - self.core), (self.right, self.core), (self.left, self.core)]
        for peer in peers:
            pl.semaphore_signal(barrier, inc=1, device_id=self.to(*peer), device_id_type=MESH)
        pl.semaphore_wait(barrier, len(peers))

    def swap(self, u, slot):
        rows = self.share * self.chips
        other = pl.ds(pl.multiple_of((1 - self.core) * rows, rows), rows)
        return pltpu.make_async_remote_copy(
            src_ref=self.g_buf.at[slot, other],
            dst_ref=self.got_half.at[u],
            send_sem=self.swap_sems.at[0, u],
            recv_sem=self.swap_sems.at[1, u],
            device_id=self.to(self.chip, 1 - self.core),
            device_id_type=MESH,
        )

    def at(self, slot, chip, top=True, bottom=True):
        start = (self.core * self.chips + chip) * self.share + (0 if top else self.share // 2)
        size = self.share if top and bottom else self.share // 2
        return self.g_buf.at[slot, pl.ds(pl.multiple_of(start, size), size)]

    def copy(self, u, slot, which):
        top, bottom = pl.ds(0, self.share // 2), pl.ds(self.share // 2, self.share // 2)
        source, target, chip = {
            0: (self.at(slot, self.far, bottom=False), self.got_far.at[u, 0], self.right),
            1: (self.at(slot, self.far, top=False), self.got_far.at[u, 1], self.left),
            2: (self.at(slot, self.right, top=False), self.got_near.at[u, 0, bottom], self.right),
            3: (self.at(slot, self.left, bottom=False), self.got_near.at[u, 1, top], self.left),
            4: (self.at(slot, self.right, bottom=False), self.got_near.at[u, 0, top], self.right),
            5: (self.at(slot, self.left, top=False), self.got_near.at[u, 1, bottom], self.left),
        }[which]
        return pltpu.make_async_remote_copy(
            src_ref=source,
            dst_ref=target,
            send_sem=self.sems.at[0, u, which],
            recv_sem=self.sems.at[1, u, which],
            device_id=self.to(chip, self.core),
            device_id_type=MESH,
        )

    def first(self, u, slot):
        self.swap(u, slot).wait()
        for chip in range(self.chips):
            there = pl.ds(chip * self.share, self.share)
            mine = self.at(slot, chip)
            mine[...] = (mine[...].astype(F32) + self.got_half[u, there, :].astype(F32)).astype(BF16)
        for which in range(4):
            self.copy(u, slot, which).start()

    def second(self, u, slot):
        for which, mine in ((0, self.at(slot, self.right, bottom=False)), (1, self.at(slot, self.left, top=False))):
            self.copy(u, slot, which).wait_recv()
            mine[...] = (mine[...].astype(F32) + self.got_far[u, which].astype(F32)).astype(BF16)
            self.copy(u, slot, which + 4).start()

    def third(self, u, slot):
        for which in range(2, 6):
            self.copy(u, slot, which).wait_recv()
        total = self.at(slot, self.chip)[...].astype(F32) + self.got_near[u, 0].astype(F32) + self.got_near[u, 1].astype(F32)
        total = total.astype(BF16)
        self.own_ref[u] = total
        wide = total.astype(F32)
        wide = (wide * wide).reshape(-1, 8, wide.shape[-1]).sum(0)
        self.squares[...] += sum(wide[:, i : i + 128] for i in range(0, wide.shape[-1], 128))
        for which in range(6):
            self.copy(u, slot, which).wait_send()


def backward_kernel(n, with_da, h_ref, dy_ref, wg_ref, wu_ref, wd_ref, *refs):
    outs = 3 if with_da else 2
    own_ref, squares_ref = refs[0], refs[1]
    a_buf, at_buf, dyt_buf, gu_buf, act_buf, acc = refs[outs : outs + 6]
    g_buf, got_half, got_far, got_near, *sems = refs[outs + 6 :]
    s = pl.program_id(0)
    last = pl.num_programs(0) - 1
    tokens, d = a_buf.shape
    chunks = [pl.ds(t, CHUNK) for t in range(0, tokens, CHUNK)]
    ex = Exchange(n, g_buf, got_half, got_far, got_near, own_ref, squares_ref, sems)

    @pl.when(s == 0)
    def _():
        ex.barrier()
        squares_ref[...] = jnp.zeros_like(squares_ref)
        for rows in chunks:
            a = normed(h_ref[0, rows, :])
            a_buf[rows, :] = a
            at_buf[:, rows] = a.T
            dyt_buf[:, rows] = dy_ref[0, rows, :].T
            if with_da:
                acc[rows, :] = jnp.zeros((CHUNK, d), F32)

    before = 3 * (s - 1)

    def tick(t):
        @pl.when(s > 0)
        def _():
            if t == 0:
                ex.first(before + 2, 2)
                ex.second(before, 0)
            if t == 1:
                ex.second(before + 1, 1)
            if t == 2:
                ex.second(before + 2, 2)
                ex.third(before, 0)
            if t == 3:
                ex.third(before + 1, 1)
                ex.third(before + 2, 2)

    for t, rows in enumerate(chunks):
        tick(t)
        a = a_buf[rows, :]
        gate = dot(a, wg_ref[0])
        up = dot(a, wu_ref[0])
        dact = dot_nt(dy_ref[0, rows, :], wd_ref[0]).astype(BF16).astype(F32)
        sig = jax.nn.sigmoid(gate)
        silu = gate * sig
        act_buf[rows, :] = (silu * up).astype(BF16)
        dup = (dact * silu).astype(BF16)
        dgate = (dact * up * (sig + silu * (1 - sig))).astype(BF16)
        gu_buf[0, rows, :] = dgate
        gu_buf[1, rows, :] = dup
        if with_da:
            acc[rows, :] += dot_nt(dgate, wg_ref[0]) + dot_nt(dup, wu_ref[0])

    for j, (left, right) in enumerate(((at_buf, gu_buf.at[0]), (at_buf, gu_buf.at[1]), (dyt_buf, act_buf))):

        def weights(i, _):
            rows = pl.ds(pl.multiple_of(i * ROWS, ROWS), ROWS)
            g_buf[j, rows, :] = dot(left[rows, :], right[...]).astype(BF16)
            return 0

        lax.fori_loop(0, d // ROWS, weights, 0)
        ex.swap(3 * s + j, j).start()
        if j > 0:
            ex.first(3 * s + j - 1, j - 1)

    @pl.when(s == last)
    def _():
        u = 3 * s
        ex.first(u + 2, 2)
        ex.second(u, 0)
        if with_da:
            dh_ref = refs[2]
            for rows in chunks:
                wide = h_ref[0, rows, :].astype(F32)
                scale = norm_scale(wide)
                da = acc[rows, :].astype(BF16).astype(F32)
                by_h = da * scale - wide * (scale * scale * scale * jnp.mean(da * wide, -1, keepdims=True))
                dh_ref[0, rows, :] = dy_ref[0, rows, :] + by_h.astype(BF16)
        ex.second(u + 1, 1)
        ex.second(u + 2, 2)
        for j in range(3):
            ex.third(u + j, j)


def backward(n, layer, with_da, h, dy, weights):
    _, tokens, d = h.shape
    ff = weights[0].shape[-1]
    units = 3 * (ff // WIDTH)
    share, chips = d // n, n // 2
    out_shape = [jax.ShapeDtypeStruct((units, share, WIDTH), BF16), jax.ShapeDtypeStruct((8, 128), F32)]
    if with_da:
        out_shape.append(jax.ShapeDtypeStruct(h.shape, BF16))
    return pl.pallas_call(
        functools.partial(backward_kernel, n, with_da),
        grid=(ff // WIDTH,),
        in_specs=[once(h.shape), once(h.shape)] + weight_specs(layer, d),
        out_specs=[once(o.shape) for o in out_shape],
        out_shape=out_shape,
        scratch_shapes=[
            pltpu.VMEM((tokens, d), BF16),
            pltpu.VMEM((d, tokens), BF16),
            pltpu.VMEM((d, tokens), BF16),
            pltpu.VMEM((2, tokens, WIDTH), BF16),
            pltpu.VMEM((tokens, WIDTH), BF16),
            pltpu.VMEM((tokens, d) if with_da else (8, 128), F32),
            pltpu.VMEM((3, d, WIDTH), BF16),
            pltpu.VMEM((units, chips * share, WIDTH), BF16),
            pltpu.VMEM((units, 2, share // 2, WIDTH), BF16),
            pltpu.VMEM((units, 2, share, WIDTH), BF16),
            pltpu.SemaphoreType.DMA((2, units)),
            pltpu.SemaphoreType.DMA((2, units, 6)),
        ],
        compiler_params=pltpu.CompilerParams(
            vmem_limit_bytes=VMEM_LIMIT, dimension_semantics=("arbitrary",), collective_id=1 + layer, has_side_effects=True
        ),
        name=f"backward_{layer}",
    )(h, dy, *weights)


def adamw_kernel(f_ref, g_ref, *refs):
    ws, ms, vs = refs[0:3], refs[3:6], refs[6:9]
    new_ws, new_ms, new_vs = refs[9:12], refs[12:15], refs[15:18]
    factor = f_ref[0]
    n, _, share, _ = g_ref.shape

    def update(g, w, m, v, new_w, new_m, new_v, rows, columns):
        at = (0, rows, columns)
        g = g * factor
        m = 0.9 * m[at] + 0.1 * g
        v = 0.95 * v[at] + 0.05 * g * g
        new_m[at] = m
        new_v[at] = v
        wide = w[at].astype(F32)
        new_w[at] = (wide - 0.02 * (m * lax.rsqrt(v + 1e-8) + 0.1 * wide)).astype(BF16)

    everything = list(zip(ws, ms, vs, new_ws, new_ms, new_vs, strict=True))
    place = {i: ((i % 2) * (n // 2) + i // 2) * share for i in range(n)}
    for j in range(2):
        for i, row in place.items():
            update(g_ref[i, j].astype(F32), *everything[j], slice(row, row + share), slice(None))
    order = sorted(place, key=place.get)
    half = n // 2
    for i in range(0, n, half):
        part = jnp.concatenate([g_ref[k, 2] for k in order[i : i + half]], 0).astype(F32)
        update(part.T, *everything[2], slice(None), slice(i * share, (i + half) * share))


def adamw(factor, layer, g, weights, m, v, earlier):
    layers, d, ff = weights[0].shape
    n, units, share, _ = g.shape
    wide = pl.BlockSpec((1, d, STRIP), lambda s: (layer, 0, s))
    tall = pl.BlockSpec((1, STRIP, d), lambda s: (layer, s, 0))
    three = [wide, wide, tall]
    strips = WIDTH // STRIP
    anywhere = [pl.BlockSpec(memory_space=pl.ANY)] * len(earlier)

    def kernel(f_ref, g_ref, *refs):
        adamw_kernel(f_ref, g_ref, *refs[:9], *refs[9 + len(earlier) :])

    return pl.pallas_call(
        kernel,
        grid=(ff // STRIP,),
        in_specs=[pl.BlockSpec(memory_space=pltpu.SMEM), pl.BlockSpec((n, 3, share, STRIP), lambda s: (0, s // strips, 0, s % strips))] + three * 3 + anywhere,
        out_specs=three * 3,
        out_shape=[jax.ShapeDtypeStruct(w.shape, t) for t in (BF16, F32, F32) for w in weights],
        input_output_aliases={11 + i: i for i in range(len(earlier))},
        compiler_params=pltpu.CompilerParams(vmem_limit_bytes=VMEM_LIMIT, dimension_semantics=("arbitrary",)),
        name=f"adamw_{layer}",
    )(factor, g, *weights, *m, *v, *earlier)


def solution(mesh):
    n = mesh.shape["dp"]

    def step(x, dy, *arrays):
        weights, m, v = (arrays[i : i + 3] for i in (0, 3, 6))
        layers = weights[0].shape[0]
        kept = [x]
        for number in range(layers - 1):
            kept.append(forward(number, kept[-1], weights))
        by_h, own, squares = dy, [None] * layers, []
        for number in reversed(range(layers)):
            own[number], part, *rest = backward(n, number, number > 0, kept[number], by_h, weights)
            squares.append(part)
            if rest:
                by_h = rest[0]
        count = sum(w.size for w in weights)
        total = lax.psum(sum(jnp.sum(part) for part in squares), "dp")
        factor = jnp.minimum(1.0, 0.5 * lax.rsqrt(total / count + 1e-30)).reshape(1)
        new = []
        for number in reversed(range(layers)):
            g = lax.all_gather(own[number], "dp")
            new = adamw(factor, number, g, weights, m, v, new)
        return tuple(new)

    return jax.shard_map(
        step,
        mesh=mesh,
        in_specs=(P(("rep", "dp"), None, None),) * 2 + (P(None, None, None),) * 9,
        out_specs=(P("rep", None, None),) * 9,
        check_vma=False,
    )
```

```python
import functools

import jax
import jax.numpy as jnp
from jax import lax
from jax.experimental import pallas as pl
from jax.experimental.pallas import tpu as pltpu
from jax.sharding import PartitionSpec as P

F32, BF16 = jnp.float32, jnp.bfloat16
MESH = pl.DeviceIdType.MESH
WIDTH = 768
STRIP = 256
CHUNK = 512
ROWS = 256
VMEM_LIMIT = 63 * 1024 * 1024
NT = (((1,), (1,)), ((), ()))


def dot(a, b):
    return jnp.dot(a, b, preferred_element_type=F32)


def dot_nt(a, b):
    return lax.dot_general(a, b, NT, preferred_element_type=F32)


def norm_scale(wide):
    return lax.rsqrt(jnp.mean(wide**2, -1, keepdims=True) + 1e-6)


def normed(h):
    wide = h.astype(F32)
    return (wide * norm_scale(wide)).astype(BF16)


def once(shape):
    return pl.BlockSpec(shape, lambda *_: (0,) * len(shape), pipeline_mode=pl.Buffered(1))


def forward_kernel(h_ref, wg_ref, wu_ref, wd_ref, out_ref, a_buf, acc):
    s = pl.program_id(0)
    tokens = a_buf.shape[0]
    chunks = [pl.ds(t, CHUNK) for t in range(0, tokens, CHUNK)]

    @pl.when(s == 0)
    def _():
        for rows in chunks:
            a_buf[rows, :] = normed(h_ref[0, rows, :])
            acc[rows, :] = jnp.zeros((CHUNK, acc.shape[1]), F32)

    for rows in chunks:
        a = a_buf[rows, :]
        gate = dot(a, wg_ref[0])
        up = dot(a, wu_ref[0])
        act = (gate * jax.nn.sigmoid(gate) * up).astype(BF16)
        acc[rows, :] += dot(act, wd_ref[0])

    @pl.when(s == pl.num_programs(0) - 1)
    def _():
        for rows in chunks:
            out_ref[0, rows, :] = h_ref[0, rows, :] + acc[rows, :].astype(BF16)


def weight_specs(layer, d):
    wide = pl.BlockSpec((1, d, WIDTH), lambda s: (layer, 0, s))
    return [wide, wide, pl.BlockSpec((1, WIDTH, d), lambda s: (layer, s, 0))]


def forward(layer, h, weights):
    _, tokens, d = h.shape
    ff = weights[0].shape[-1]
    return pl.pallas_call(
        forward_kernel,
        grid=(ff // WIDTH,),
        in_specs=[once(h.shape)] + weight_specs(layer, d),
        out_specs=once(h.shape),
        out_shape=jax.ShapeDtypeStruct(h.shape, BF16),
        scratch_shapes=[pltpu.VMEM((tokens, d), BF16), pltpu.VMEM((tokens, d), F32)],
        compiler_params=pltpu.CompilerParams(vmem_limit_bytes=VMEM_LIMIT, dimension_semantics=("arbitrary",)),
        name="forward",
    )(h, *weights)


class Exchange:
    def __init__(self, n, g_buf, got_half, got_far, got_near, own_ref, squares, sems):
        self.g_buf, self.got_half, self.got_far, self.got_near = g_buf, got_half, got_far, got_near
        self.own_ref, self.squares = own_ref, squares
        self.swap_sems, self.sems = sems
        me = lax.axis_index("dp")
        self.core, self.chip = lax.rem(me, 2), me // 2
        self.chips = n // 2
        self.right = lax.rem(self.chip + 1, self.chips)
        self.left = lax.rem(self.chip + self.chips - 1, self.chips)
        self.far = lax.rem(self.chip + 2, self.chips)
        self.row = (self.core * self.chips + self.chip) * got_near.shape[2]
        self.share = got_near.shape[2]

    def to(self, chip, core):
        return {"dp": chip * 2 + core}

    def barrier(self, far):
        barrier = pltpu.get_barrier_semaphore()
        peers = [(self.chip, 1 - self.core), (self.right, self.core), (self.left, self.core)]
        if far:
            peers.append((self.far, self.core))
        for peer in peers:
            pl.semaphore_signal(barrier, inc=1, device_id=self.to(*peer), device_id_type=MESH)
        pl.semaphore_wait(barrier, len(peers))

    def swap(self, u, slot):
        rows = self.share * self.chips
        other = pl.ds(pl.multiple_of((1 - self.core) * rows, rows), rows)
        return pltpu.make_async_remote_copy(
            src_ref=self.g_buf.at[slot, other],
            dst_ref=self.got_half.at[u],
            send_sem=self.swap_sems.at[0, u],
            recv_sem=self.swap_sems.at[1, u],
            device_id=self.to(self.chip, 1 - self.core),
            device_id_type=MESH,
        )

    def at(self, slot, chip, top=True, bottom=True):
        start = (self.core * self.chips + chip) * self.share + (0 if top else self.share // 2)
        size = self.share if top and bottom else self.share // 2
        return self.g_buf.at[slot, pl.ds(pl.multiple_of(start, size), size)]

    def copy(self, u, slot, which):
        top, bottom = pl.ds(0, self.share // 2), pl.ds(self.share // 2, self.share // 2)
        source, target, chip = {
            0: (self.at(slot, self.far, bottom=False), self.got_far.at[u, 0], self.right),
            1: (self.at(slot, self.far, top=False), self.got_far.at[u, 1], self.left),
            2: (self.at(slot, self.right, top=False), self.got_near.at[u, 0, bottom], self.right),
            3: (self.at(slot, self.left, bottom=False), self.got_near.at[u, 1, top], self.left),
            4: (self.at(slot, self.right, bottom=False), self.got_near.at[u, 0, top], self.right),
            5: (self.at(slot, self.left, top=False), self.got_near.at[u, 1, bottom], self.left),
        }[which]
        return pltpu.make_async_remote_copy(
            src_ref=source,
            dst_ref=target,
            send_sem=self.sems.at[0, u, which],
            recv_sem=self.sems.at[1, u, which],
            device_id=self.to(chip, self.core),
            device_id_type=MESH,
        )

    def first(self, u, slot):
        self.swap(u, slot).wait()
        for chip in range(self.chips):
            there = pl.ds(chip * self.share, self.share)
            mine = self.at(slot, chip)
            mine[...] = (mine[...].astype(F32) + self.got_half[u, there, :].astype(F32)).astype(BF16)
        for which in range(4):
            self.copy(u, slot, which).start()

    def second(self, u, slot):
        for which, mine in ((0, self.at(slot, self.right, bottom=False)), (1, self.at(slot, self.left, top=False))):
            self.copy(u, slot, which).wait_recv()
            mine[...] = (mine[...].astype(F32) + self.got_far[u, which].astype(F32)).astype(BF16)
            self.copy(u, slot, which + 4).start()

    def third(self, u, slot):
        for which in range(2, 6):
            self.copy(u, slot, which).wait_recv()
        total = self.at(slot, self.chip)[...].astype(F32) + self.got_near[u, 0].astype(F32) + self.got_near[u, 1].astype(F32)
        total = total.astype(BF16)
        self.own_ref[u] = total
        wide = total.astype(F32)
        wide = (wide * wide).reshape(-1, 8, wide.shape[-1]).sum(0)
        self.squares[...] += sum(wide[:, i : i + 128] for i in range(0, wide.shape[-1], 128))
        for which in range(6):
            self.copy(u, slot, which).wait_send()


class Gather:
    def __init__(self, ex, own_ref, first, g_ref, sems, local_sem):
        self.ex, self.own_ref, self.first, self.g_ref, self.sems, self.local_sem = ex, own_ref, first, g_ref, sems, local_sem

    def rows(self, u, chip, top=True, bottom=True):
        ex = self.ex
        start = (ex.core * ex.chips + chip) * ex.share + (0 if top else ex.share // 2)
        size = ex.share if top and bottom else ex.share // 2
        return self.g_ref.at[u, pl.ds(pl.multiple_of(start, size), size)]

    def copy(self, u, which):
        ex = self.ex
        here = (ex.chip, 1 - ex.core)
        mine = self.rows(u, ex.chip)
        source, target, to = {
            0: (self.own_ref.at[self.first + u], mine, (ex.right, ex.core)),
            1: (self.own_ref.at[self.first + u], mine, (ex.left, ex.core)),
            2: (self.own_ref.at[self.first + u], mine, here),
            3: (self.rows(u, ex.left, bottom=False),) * 2 + ((ex.right, ex.core),),
            4: (self.rows(u, ex.right, top=False),) * 2 + ((ex.left, ex.core),),
            5: (self.rows(u, ex.left),) * 2 + (here,),
            6: (self.rows(u, ex.right),) * 2 + (here,),
            7: (self.rows(u, ex.far, bottom=False),) * 2 + (here,),
            8: (self.rows(u, ex.far, top=False),) * 2 + (here,),
        }[which]
        return pltpu.make_async_remote_copy(
            src_ref=source,
            dst_ref=target,
            send_sem=self.sems.at[0, u, which],
            recv_sem=self.sems.at[1, u, which],
            device_id=ex.to(*to),
            device_id_type=MESH,
        )

    def local(self, u):
        return pltpu.make_async_copy(self.own_ref.at[self.first + u], self.rows(u, self.ex.chip), self.local_sem.at[u])

    def one(self, u):
        for which in range(3):
            self.copy(u, which).start()
        self.local(u).start()

    def two(self, u):
        for which in range(2):
            self.copy(u, which).wait_recv()
            self.copy(u, which + 3).start()
            self.copy(u, which + 5).start()

    def three(self, u):
        for which in range(2):
            self.copy(u, which + 3).wait_recv()
            self.copy(u, which + 7).start()

    def four(self, u):
        for which in (2, 5, 6, 7, 8):
            self.copy(u, which).wait_recv()
        for which in range(9):
            self.copy(u, which).wait_send()
        self.local(u).wait()


def squares_over_group(ex, squares_ref, slots, sems):
    def send(slot, which, chip, core):
        return pltpu.make_async_remote_copy(
            src_ref=slots.at[slot],
            dst_ref=slots.at[5 if which == 0 else 1 + ex.chip],
            send_sem=sems.at[0, which],
            recv_sem=sems.at[1, which],
            device_id=ex.to(chip, core),
            device_id_type=MESH,
        )

    slots[0] = squares_ref[...]
    swap = send(0, 0, ex.chip, 1 - ex.core)
    swap.start()
    swap.wait()
    slots[1 + ex.chip] = slots[0] + slots[5]
    copies = [send(1 + ex.chip, 1 + i, chip, ex.core) for i, chip in enumerate((ex.right, ex.left, ex.far))]
    for copy in copies:
        copy.start()
    for copy in copies:
        copy.wait()
    total = slots[1]
    for chip in range(1, ex.chips):
        total = total + slots[1 + chip]
    squares_ref[...] = total


def backward_kernel(n, with_da, h_ref, dy_ref, wg_ref, wu_ref, wd_ref, *refs):
    if with_da:
        own_ref, squares_ref, gathered_ref, dh_ref, *refs = refs
    else:
        earlier_own_ref, earlier_squares_ref, own_ref, squares_ref, gathered_ref, *refs = refs
    a_buf, t_buf, gu_buf, acc, g_buf, got_half, got_far, got_near, slots, *sems = refs
    swap_sems, copy_sems, gather_sems, local_sems, slot_sems = sems
    s = pl.program_id(0)
    last = pl.num_programs(0) - 1
    tokens, d = a_buf.shape
    steps = tokens // CHUNK
    ex = Exchange(n, g_buf, got_half, got_far, got_near, own_ref, squares_ref, (swap_sems, copy_sems))
    gather = Gather(ex, own_ref if with_da else earlier_own_ref, 0, gathered_ref, gather_sems, local_sems)

    def chunk(t):
        return pl.ds(pl.multiple_of(t * CHUNK, CHUNK), CHUNK)

    def each(f, start=0):
        lax.fori_loop(0, 3, lambda j, _: (f(start + j), 0)[1], 0)

    @pl.when(s == 0)
    def _():
        ex.barrier(not with_da)
        if with_da:
            squares_ref[...] = jnp.zeros_like(squares_ref)
        else:
            squares_ref[...] = earlier_squares_ref[...]
            each(gather.one)

        def prepare(t, _):
            rows = chunk(t)
            a = normed(h_ref[0, rows, :])
            a_buf[rows, :] = a
            t_buf[0, :, rows] = a.T
            t_buf[1, :, rows] = dy_ref[0, rows, :].T
            if with_da:
                acc[rows, :] = jnp.zeros((CHUNK, d), F32)
            return 0

        lax.fori_loop(0, steps, prepare, 0)

    def due(u, what):
        steps = {"f": ex.first, "s": ex.second, "t": ex.third}
        gathers = {"1": gather.one, "2": gather.two, "3": gather.three, "4": gather.four}
        for step, j in zip(what[::2], map(int, what[1::2])):
            if step in steps:
                steps[step](u + j, j)
            else:
                gathers[step](u + j)

    here, before = 3 * s, 3 * (s - 1)

    def when(condition, *actions):
        @pl.when(condition)
        def _():
            for action in actions:
                action()

    if with_da:
        in_hidden = {0: "s1", 1: "s2", 2: "t010", 3: "t111"}
        in_weights = {0: "t212", 1: "20", 2: "21"}
        in_da = {1: "f2", 2: "s0"}
        before_in_da = {0: "2230", 2: "31"}
        earlier_in_hidden = {0: "32", 3: "404142"}
        at_last, before_at_last = "s1s2t0t1t2", "32404142"
    else:
        in_hidden = {1: "f2s0", 2: "s1"}
        in_weights = {0: "s2t0", 1: "t1", 2: "t2"}
        earlier_in_hidden = {}
        at_last = "s0f2s1t0s2t1t2"

    def hidden(t, _):
        for i, what in in_hidden.items():
            when((s > 0) & (t == i), functools.partial(due, before, what))
        for i, what in earlier_in_hidden.items():
            when((s > 1) & (t == i), functools.partial(due, before - 3, what))
        if not with_da:
            when((s == 0) & (t == 1), functools.partial(due, 0, "20"))
            when((s == 0) & (t == 2), functools.partial(due, 0, "21"))
            when((s == 0) & (t == 3), functools.partial(due, 0, "2230"))
            when((s == 1) & (t == 0), functools.partial(due, 0, "3132404142"))
        rows = chunk(t)
        a = a_buf[rows, :]
        gate = dot(a, wg_ref[0])
        up = dot(a, wu_ref[0])
        dact = dot_nt(dy_ref[0, rows, :], wd_ref[0]).astype(BF16).astype(F32)
        sig = jax.nn.sigmoid(gate)
        silu = gate * sig
        gu_buf[0, rows, :] = (dact * up * (sig + silu * (1 - sig))).astype(BF16)
        gu_buf[1, rows, :] = (dact * silu).astype(BF16)
        gu_buf[2, rows, :] = (silu * up).astype(BF16)
        return 0

    lax.fori_loop(0, steps, hidden, 0)

    def weights(j, _):
        for i, what in in_weights.items():
            when((s > 0) & (j == i), functools.partial(due, before, what))
        g_buf[j] = dot(t_buf[j // 2], gu_buf[j]).astype(BF16)
        ex.swap(here + j, j).start()
        when(j > 0, lambda: ex.first(here + j - 1, j - 1))
        return 0

    lax.fori_loop(0, 3, weights, 0)

    if with_da:

        def by_a(t, _):
            for i, what in in_da.items():
                when(t == i, functools.partial(due, here, what))
            for i, what in before_in_da.items():
                when((s > 0) & (t == i), functools.partial(due, before, what))
            rows = chunk(t)
            acc[rows, :] += dot_nt(gu_buf[0, rows, :], wg_ref[0]) + dot_nt(gu_buf[1, rows, :], wu_ref[0])
            return 0

        lax.fori_loop(0, steps, by_a, 0)

    @pl.when(s == last)
    def _():
        if with_da:

            def by_h(t, _):
                rows = chunk(t)
                wide = h_ref[0, rows, :].astype(F32)
                scale = norm_scale(wide)
                da = acc[rows, :].astype(BF16).astype(F32)
                through = da * scale - wide * (scale * scale * scale * jnp.mean(da * wide, -1, keepdims=True))
                dh_ref[0, rows, :] = dy_ref[0, rows, :] + through.astype(BF16)
                return 0

            lax.fori_loop(0, steps, by_h, 0)
        due(here, at_last)
        if with_da:
            due(before, before_at_last)
        else:
            squares_over_group(ex, squares_ref, slots, slot_sems)


def backward(n, layer, with_da, h, dy, weights, earlier=()):
    _, tokens, d = h.shape
    ff = weights[0].shape[-1]
    units = 3 * (ff // WIDTH)
    share, chips = d // n, n // 2
    gathered = units - 3 if with_da else 3
    out_shape = [
        jax.ShapeDtypeStruct((units, share, WIDTH), BF16),
        jax.ShapeDtypeStruct((8, 128), F32),
        jax.ShapeDtypeStruct((gathered, d, WIDTH), BF16),
    ]
    out_specs = [once(out_shape[0].shape), once(out_shape[1].shape), pl.BlockSpec(memory_space=pl.ANY)]
    if with_da:
        out_shape.append(jax.ShapeDtypeStruct(h.shape, BF16))
        out_specs.append(once(h.shape))
        more = []
    else:
        last = units // 3 - 1
        more = [pl.BlockSpec((3, share, WIDTH), lambda s: (last, 0, 0), pipeline_mode=pl.Buffered(1)), once((8, 128))]
    return pl.pallas_call(
        functools.partial(backward_kernel, n, with_da),
        grid=(ff // WIDTH,),
        in_specs=[once(h.shape), once(h.shape)] + weight_specs(layer, d) + more,
        out_specs=out_specs,
        out_shape=out_shape,
        scratch_shapes=[
            pltpu.VMEM((tokens, d), BF16),
            pltpu.VMEM((2, d, tokens), BF16),
            pltpu.VMEM((3, tokens, WIDTH), BF16),
            pltpu.VMEM((tokens, d) if with_da else (8, 128), F32),
            pltpu.VMEM((3, d, WIDTH), BF16),
            pltpu.VMEM((units, chips * share, WIDTH), BF16),
            pltpu.VMEM((units, 2, share // 2, WIDTH), BF16),
            pltpu.VMEM((units, 2, share, WIDTH), BF16),
            pltpu.VMEM((chips + 2, 8, 128), F32),
            pltpu.SemaphoreType.DMA((2, units)),
            pltpu.SemaphoreType.DMA((2, units, 6)),
            pltpu.SemaphoreType.DMA((2, gathered, 9)),
            pltpu.SemaphoreType.DMA((gathered,)),
            pltpu.SemaphoreType.DMA((2, 4)),
        ],
        compiler_params=pltpu.CompilerParams(
            vmem_limit_bytes=VMEM_LIMIT, dimension_semantics=("arbitrary",), collective_id=1 + layer, has_side_effects=True
        ),
        name=f"backward_{layer}",
    )(h, dy, *weights, *earlier)


def adamw_kernel(count, rows_ref, q_ref, pieces, refs):
    ws, ms, vs = refs[0:3], refs[3:6], refs[6:9]
    new_ws, new_ms, new_vs = refs[9:12], refs[12:15], refs[15:18]
    factor = jnp.minimum(1.0, 0.5 * lax.rsqrt(jnp.full((1, 1), jnp.sum(q_ref[...]) / count, F32) + 1e-30))

    def update(g, w, m, v, new_w, new_m, new_v, rows, columns):
        at = (0, rows, columns)
        g = g * factor
        m = 0.9 * m[at] + 0.1 * g
        v = 0.95 * v[at] + 0.05 * g * g
        new_m[at] = m
        new_v[at] = v
        wide = w[at].astype(F32)
        new_w[at] = (wide - 0.02 * (m * lax.rsqrt(v + 1e-8) + 0.1 * wide)).astype(BF16)

    everything = list(zip(ws, ms, vs, new_ws, new_ms, new_vs, strict=True))
    g_ref = pieces[0]
    if len(pieces) > 1:
        g_ref = refs[18]
        for i, piece in enumerate(pieces):
            size = piece.shape[1]
            for j in range(3):
                g_ref[j, pl.ds(pl.multiple_of(rows_ref[i], size), size), :] = piece[j]
    d = g_ref.shape[1]
    for j in range(2):
        for row in range(0, d, 192):
            rows = slice(row, row + 192)
            update(g_ref[j, rows, :].astype(F32), *everything[j], rows, slice(None))
    for row in range(0, d, 384):
        rows = slice(row, row + 384)
        update(g_ref[2, rows, :].astype(F32).T, *everything[2], slice(None), rows)


def adamw(squares, layer, slices, pieces, rows, weights, m, v, earlier):
    layers, d, ff = weights[0].shape
    strips = WIDTH // STRIP
    start = slices[0] * strips
    wide = pl.BlockSpec((1, d, STRIP), lambda s: (layer, 0, start + s))
    tall = pl.BlockSpec((1, STRIP, d), lambda s: (layer, start + s, 0))
    three = [wide, wide, tall]
    anywhere = [pl.BlockSpec(memory_space=pl.ANY)] * len(earlier)
    count = sum(w.size for w in weights)
    k, parts = len(pieces), slices[1] - slices[0]

    def kernel(rows_ref, q_ref, *refs):
        refs = refs[: k + 9] + refs[k + 9 + len(earlier) :]
        adamw_kernel(count, rows_ref, q_ref, refs[:k], refs[k:])

    return pl.pallas_call(
        kernel,
        grid=(parts * strips,),
        in_specs=[pl.BlockSpec(memory_space=pltpu.SMEM), once((8, 128))]
        + [pl.BlockSpec((3, g.shape[1], STRIP), lambda s: (s // strips, 0, s % strips)) for g in pieces]
        + three * 3
        + anywhere,
        out_specs=three * 3,
        out_shape=[jax.ShapeDtypeStruct(w.shape, t) for t in (BF16, F32, F32) for w in weights],
        scratch_shapes=[pltpu.VMEM((3, d, STRIP), BF16)] if k > 1 else [],
        input_output_aliases={11 + k + i: i for i in range(len(earlier))},
        compiler_params=pltpu.CompilerParams(vmem_limit_bytes=VMEM_LIMIT, dimension_semantics=("arbitrary",)),
        cost_estimate=pl.CostEstimate(flops=10**11 // 6 * parts, bytes_accessed=39 * 10**6 * parts, transcendentals=0),
        name=f"adamw_{layer}_{slices[0]}",
    )(rows, squares, *pieces, *weights, *m, *v, *earlier)


def gathered(n, own, first, second):
    chips, share = n // 2, own.shape[1]
    half = share // 2
    me = lax.axis_index("dp")
    core, chip = me % 2, me // 2
    left, right, far = (chip + chips - 1) % chips, (chip + 1) % chips, (chip + 2) % chips

    def shift(a, by):
        return lax.ppermute(a, "dp", [(c * 2 + k, (c + by) % chips * 2 + k) for c in range(chips) for k in range(2)])

    def swap(a):
        return lax.ppermute(a, "dp", [(i, i ^ 1) for i in range(n)])

    from_left, from_right = shift(own, 1), shift(own, -1)
    result = first()
    from_left, from_right, result = lax.optimization_barrier((from_left, from_right, result))
    far_top, far_bottom = shift(from_left[:, :half], 1), shift(from_right[:, half:], -1)
    near = [own, from_left, from_right]
    near_there = [swap(piece) for piece in near]
    result = second(result)
    far_top, far_bottom, result = lax.optimization_barrier((far_top, far_bottom, result))
    pieces = near + [far_top, far_bottom] + near_there + [swap(far_top), swap(far_bottom)]
    rows = [chip * share, left * share, right * share, far * share, far * share + half]
    rows = [core * chips * share + row for row in rows] + [(1 - core) * chips * share + row for row in rows]
    return pieces, jnp.stack(rows).astype(jnp.int32), result


def solution(mesh):
    n = mesh.shape["dp"]

    def step(x, dy, *arrays):
        weights, m, v = (arrays[i : i + 3] for i in (0, 3, 6))
        slices = weights[0].shape[-1] // WIDTH
        h = forward(0, x, weights)
        own_1, squares, g_1, dh = backward(n, 1, True, h, dy, weights)
        own_0, squares, g_1_last = backward(n, 0, False, x, dh, weights, (own_1, squares))
        nowhere = jnp.zeros((1,), jnp.int32)
        pieces, rows, new = gathered(
            n,
            own_0,
            lambda: adamw(squares, 1, (0, slices - 1), [g_1], nowhere, weights, m, v, ()),
            lambda new: adamw(squares, 1, (slices - 1, slices), [g_1_last], nowhere, weights, m, v, new),
        )
        return tuple(adamw(squares, 0, (0, slices), pieces, rows, weights, m, v, new))

    return jax.shard_map(
        step,
        mesh=mesh,
        in_specs=(P(("rep", "dp"), None, None),) * 2 + (P(None, None, None),) * 9,
        out_specs=(P("rep", None, None),) * 9,
        check_vma=False,
    )
```

```python
import functools

import jax
import jax.numpy as jnp
from jax import lax
from jax.experimental import pallas as pl
from jax.experimental.pallas import tpu as pltpu
from jax.sharding import PartitionSpec as P

F32, BF16 = jnp.float32, jnp.bfloat16
MESH = pl.DeviceIdType.MESH
WIDTH = 768
STRIP = 256
CHUNK = 512
SLOTS = 6
VMEM_LIMIT = 63 * 1024 * 1024
NT = (((1,), (1,)), ((), ()))


def dot(a, b):
    return jnp.dot(a, b, preferred_element_type=F32)


def dot_nt(a, b):
    return lax.dot_general(a, b, NT, preferred_element_type=F32)


def norm_scale(wide):
    return lax.rsqrt(jnp.mean(wide**2, -1, keepdims=True) + 1e-6)


def normed(h):
    wide = h.astype(F32)
    return (wide * norm_scale(wide)).astype(BF16)


def once(shape):
    return pl.BlockSpec(shape, lambda *_: (0,) * len(shape), pipeline_mode=pl.Buffered(1))


def forward_kernel(h_ref, wg_ref, wu_ref, wd_ref, out_ref, gate_hbm, up_hbm, a_buf, acc, stage, sems):
    s = pl.program_id(0)
    tokens = a_buf.shape[0]
    steps = tokens // CHUNK
    count = pl.num_programs(0) * steps

    def chunk(t):
        return pl.ds(pl.multiple_of(t * CHUNK, CHUNK), CHUNK)

    def keep(step):
        slot = lax.rem(step, 2)
        return [pltpu.make_async_copy(stage.at[slot, i], to.at[step // steps, chunk(lax.rem(step, steps))], sems.at[slot, i]) for i, to in enumerate((gate_hbm, up_hbm))]

    @pl.when(s == 0)
    def _():
        def prepare(t, _):
            rows = chunk(t)
            a_buf[rows, :] = normed(h_ref[0, rows, :])
            acc[rows, :] = jnp.zeros((CHUNK, acc.shape[1]), F32)
            return 0

        lax.fori_loop(0, steps, prepare, 0)

    def hidden(t, _):
        rows, step = chunk(t), s * steps + t
        slot = lax.rem(step, 2)

        @pl.when(step >= 2)
        def _():
            for copy in keep(step - 2):
                copy.wait()

        a = a_buf[rows, :]
        gate = dot(a, wg_ref[0])
        up = dot(a, wu_ref[0])
        stage[slot, 0] = gate
        stage[slot, 1] = up
        for copy in keep(step):
            copy.start()
        act = (gate * jax.nn.sigmoid(gate) * up).astype(BF16)
        acc[rows, :] += dot(act, wd_ref[0])
        return 0

    lax.fori_loop(0, steps, hidden, 0)

    @pl.when(s == pl.num_programs(0) - 1)
    def _():
        def finish(t, _):
            rows = chunk(t)
            out_ref[0, rows, :] = h_ref[0, rows, :] + acc[rows, :].astype(BF16)
            return 0

        lax.fori_loop(0, steps, finish, 0)
        for step in (count - 2, count - 1):
            for copy in keep(step):
                copy.wait()


def weight_specs(layer, d):
    wide = pl.BlockSpec((1, d, WIDTH), lambda s: (layer, 0, s))
    return [wide, wide, pl.BlockSpec((1, WIDTH, d), lambda s: (layer, s, 0))]


def forward(layer, h, weights):
    _, tokens, d = h.shape
    ff = weights[0].shape[-1]
    kept = jax.ShapeDtypeStruct((ff // WIDTH, tokens, WIDTH), F32)
    return pl.pallas_call(
        forward_kernel,
        grid=(ff // WIDTH,),
        in_specs=[once(h.shape)] + weight_specs(layer, d),
        out_specs=[once(h.shape), pl.BlockSpec(memory_space=pl.ANY), pl.BlockSpec(memory_space=pl.ANY)],
        out_shape=[jax.ShapeDtypeStruct(h.shape, BF16), kept, kept],
        scratch_shapes=[
            pltpu.VMEM((tokens, d), BF16),
            pltpu.VMEM((tokens, d), F32),
            pltpu.VMEM((2, 2, CHUNK, WIDTH), F32),
            pltpu.SemaphoreType.DMA((2, 2)),
        ],
        compiler_params=pltpu.CompilerParams(vmem_limit_bytes=VMEM_LIMIT, dimension_semantics=("arbitrary",)),
        name="forward",
    )(h, *weights)


class Exchange:
    def __init__(self, n, g_buf, got_half, got_far, got_near, own_refs, squares, sems):
        self.g_buf, self.got_half, self.got_far, self.got_near = g_buf, got_half, got_far, got_near
        self.own_refs, self.squares = own_refs, squares
        self.swap_sems, self.sems = sems
        me = lax.axis_index("dp")
        self.core, self.chip = lax.rem(me, 2), me // 2
        self.chips = n // 2
        self.right = lax.rem(self.chip + 1, self.chips)
        self.left = lax.rem(self.chip + self.chips - 1, self.chips)
        self.far = lax.rem(self.chip + 2, self.chips)
        self.row = (self.core * self.chips + self.chip) * got_near.shape[2]
        self.share = got_near.shape[2]

    def to(self, chip, core):
        return {"dp": chip * 2 + core}

    def barrier(self, far):
        barrier = pltpu.get_barrier_semaphore()
        peers = [(self.chip, 1 - self.core), (self.right, self.core), (self.left, self.core)]
        if far:
            peers.append((self.far, self.core))
        for peer in peers:
            pl.semaphore_signal(barrier, inc=1, device_id=self.to(*peer), device_id_type=MESH)
        pl.semaphore_wait(barrier, len(peers))

    def swap(self, u, slot):
        rows = self.share * self.chips
        other = pl.ds(pl.multiple_of((1 - self.core) * rows, rows), rows)
        return pltpu.make_async_remote_copy(
            src_ref=self.g_buf.at[slot, other],
            dst_ref=self.got_half.at[u],
            send_sem=self.swap_sems.at[0, u],
            recv_sem=self.swap_sems.at[1, u],
            device_id=self.to(self.chip, 1 - self.core),
            device_id_type=MESH,
        )

    def at(self, slot, chip, top=True, bottom=True):
        start = (self.core * self.chips + chip) * self.share + (0 if top else self.share // 2)
        size = self.share if top and bottom else self.share // 2
        return self.g_buf.at[slot, pl.ds(pl.multiple_of(start, size), size)]

    def copy(self, u, slot, which):
        top, bottom = pl.ds(0, self.share // 2), pl.ds(self.share // 2, self.share // 2)
        source, target, chip = {
            0: (self.at(slot, self.far, bottom=False), self.got_far.at[u, 0], self.right),
            1: (self.at(slot, self.far, top=False), self.got_far.at[u, 1], self.left),
            2: (self.at(slot, self.right, top=False), self.got_near.at[u, 0, bottom], self.right),
            3: (self.at(slot, self.left, bottom=False), self.got_near.at[u, 1, top], self.left),
            4: (self.at(slot, self.right, bottom=False), self.got_near.at[u, 0, top], self.right),
            5: (self.at(slot, self.left, top=False), self.got_near.at[u, 1, bottom], self.left),
        }[which]
        return pltpu.make_async_remote_copy(
            src_ref=source,
            dst_ref=target,
            send_sem=self.sems.at[0, u, which],
            recv_sem=self.sems.at[1, u, which],
            device_id=self.to(chip, self.core),
            device_id_type=MESH,
        )

    def first(self, u, slot):
        self.swap(u, slot).wait()
        for chip in range(self.chips):
            there = pl.ds(chip * self.share, self.share)
            mine = self.at(slot, chip)
            mine[...] = (mine[...].astype(F32) + self.got_half[u, there, :].astype(F32)).astype(BF16)
        for which in range(4):
            self.copy(u, slot, which).start()

    def second(self, u, slot):
        for which, mine in ((0, self.at(slot, self.right, bottom=False)), (1, self.at(slot, self.left, top=False))):
            self.copy(u, slot, which).wait_recv()
            mine[...] = (mine[...].astype(F32) + self.got_far[u, which].astype(F32)).astype(BF16)
            self.copy(u, slot, which + 4).start()

    def third(self, u, slot):
        for which in range(2, 6):
            self.copy(u, slot, which).wait_recv()
        total = self.at(slot, self.chip)[...].astype(F32) + self.got_near[u, 0].astype(F32) + self.got_near[u, 1].astype(F32)
        total = total.astype(BF16)
        if len(self.own_refs) == 1:
            self.own_refs[0][u] = total
        else:
            for part, half in zip(self.own_refs, (total[: self.share // 2], total[self.share // 2 :]), strict=True):
                part[u] = half
        wide = total.astype(F32)
        wide = (wide * wide).reshape(-1, 8, wide.shape[-1]).sum(0)
        self.squares[...] += sum(wide[:, i : i + 128] for i in range(0, wide.shape[-1], 128))
        for which in range(6):
            self.copy(u, slot, which).wait_send()


class Gather:
    def __init__(self, ex, own_ref, first, g_ref, sems, local_sem):
        self.ex, self.own_ref, self.first, self.g_ref, self.sems, self.local_sem = ex, own_ref, first, g_ref, sems, local_sem

    def rows(self, u, chip, top=True, bottom=True):
        ex = self.ex
        start = (ex.core * ex.chips + chip) * ex.share + (0 if top else ex.share // 2)
        size = ex.share if top and bottom else ex.share // 2
        return self.g_ref.at[u, pl.ds(pl.multiple_of(start, size), size)]

    def copy(self, u, which):
        ex = self.ex
        here = (ex.chip, 1 - ex.core)
        mine = self.rows(u, ex.chip)
        source, target, to = {
            0: (self.own_ref.at[self.first + u], mine, (ex.right, ex.core)),
            1: (self.own_ref.at[self.first + u], mine, (ex.left, ex.core)),
            2: (self.own_ref.at[self.first + u], mine, here),
            3: (self.rows(u, ex.left, bottom=False),) * 2 + ((ex.right, ex.core),),
            4: (self.rows(u, ex.right, top=False),) * 2 + ((ex.left, ex.core),),
            5: (self.rows(u, ex.left),) * 2 + (here,),
            6: (self.rows(u, ex.right),) * 2 + (here,),
            7: (self.rows(u, ex.far, bottom=False),) * 2 + (here,),
            8: (self.rows(u, ex.far, top=False),) * 2 + (here,),
        }[which]
        return pltpu.make_async_remote_copy(
            src_ref=source,
            dst_ref=target,
            send_sem=self.sems.at[0, u, which],
            recv_sem=self.sems.at[1, u, which],
            device_id=ex.to(*to),
            device_id_type=MESH,
        )

    def local(self, u):
        return pltpu.make_async_copy(self.own_ref.at[self.first + u], self.rows(u, self.ex.chip), self.local_sem.at[u])

    def one(self, u):
        for which in range(3):
            self.copy(u, which).start()
        self.local(u).start()

    def two(self, u):
        for which in range(2):
            self.copy(u, which).wait_recv()
            self.copy(u, which + 3).start()
            self.copy(u, which + 5).start()

    def three(self, u):
        for which in range(2):
            self.copy(u, which + 3).wait_recv()
            self.copy(u, which + 7).start()

    def four(self, u):
        for which in (2, 5, 6, 7, 8):
            self.copy(u, which).wait_recv()
        for which in range(9):
            self.copy(u, which).wait_send()
        self.local(u).wait()


def squares_over_group(ex, squares_ref, slots, sems):
    def send(slot, which, chip, core):
        return pltpu.make_async_remote_copy(
            src_ref=slots.at[slot],
            dst_ref=slots.at[5 if which == 0 else 1 + ex.chip],
            send_sem=sems.at[0, which],
            recv_sem=sems.at[1, which],
            device_id=ex.to(chip, core),
            device_id_type=MESH,
        )

    slots[0] = squares_ref[...]
    swap = send(0, 0, ex.chip, 1 - ex.core)
    swap.start()
    swap.wait()
    slots[1 + ex.chip] = slots[0] + slots[5]
    copies = [send(1 + ex.chip, 1 + i, chip, ex.core) for i, chip in enumerate((ex.right, ex.left, ex.far))]
    for copy in copies:
        copy.start()
    for copy in copies:
        copy.wait()
    total = slots[1]
    for chip in range(1, ex.chips):
        total = total + slots[1 + chip]
    squares_ref[...] = total


def backward_kernel(n, with_da, h_ref, dy_ref, *refs):
    if with_da:
        wg_ref, wu_ref, wd_ref, squares_ref, gathered_ref, own_ref, dh_ref, a_buf, acc, *refs = refs
        own_refs = (own_ref,)
    else:
        wd_ref, gate_hbm, up_hbm, earlier_own_ref, earlier_squares_ref, squares_ref, gathered_ref, *own_refs, stage, stage_sems = refs[:11]
        refs = refs[11:]
    t_buf, gu_buf, g_buf, got_half, got_far, got_near, slots, *sems = refs
    swap_sems, copy_sems, gather_sems, local_sems, slot_sems = sems
    depth = g_buf.shape[0]
    s = pl.program_id(0)
    last = pl.num_programs(0) - 1
    _, tokens, d = h_ref.shape
    steps = tokens // CHUNK
    ex = Exchange(n, g_buf, got_half, got_far, got_near, own_refs, squares_ref, (swap_sems, copy_sems))
    gather = Gather(ex, own_ref if with_da else earlier_own_ref, 0, gathered_ref, gather_sems, local_sems)

    def chunk(t):
        return pl.ds(pl.multiple_of(t * CHUNK, CHUNK), CHUNK)

    def each(f, start=0):
        lax.fori_loop(0, 3, lambda j, _: (f(start + j), 0)[1], 0)

    def fetch(step):
        slot = lax.rem(step, 2)
        return [pltpu.make_async_copy(kept.at[step // steps, chunk(lax.rem(step, steps))], stage.at[slot, i], stage_sems.at[slot, i]) for i, kept in enumerate((gate_hbm, up_hbm))]

    @pl.when(s == 0)
    def _():
        if not with_da:
            for copy in fetch(0):
                copy.start()
        ex.barrier(not with_da)
        if with_da:
            squares_ref[...] = jnp.zeros_like(squares_ref)
        else:
            squares_ref[...] = earlier_squares_ref[...]
            each(gather.one)

        def prepare(t, _):
            rows = chunk(t)
            a = normed(h_ref[0, rows, :])
            t_buf[0, :, rows] = a.T
            t_buf[1, :, rows] = dy_ref[0, rows, :].T
            if with_da:
                a_buf[rows, :] = a
                acc[rows, :] = jnp.zeros((CHUNK, d), F32)
            return 0

        lax.fori_loop(0, steps, prepare, 0)

    def due(u, what):
        steps = {"f": ex.first, "s": ex.second, "t": ex.third}
        gathers = {"1": gather.one, "2": gather.two, "3": gather.three, "4": gather.four}
        for step, j in zip(what[::2], map(int, what[1::2])):
            if step in steps:
                steps[step](u + j, lax.rem(u + j, depth))
            else:
                gathers[step](u + j)

    here, before = 3 * s, 3 * (s - 1)

    def when(condition, *actions):
        @pl.when(condition)
        def _():
            for action in actions:
                action()

    if with_da:
        in_hidden = {1: "s2", 2: "t010t111", 3: "t212"}
        in_weights = {0: "20", 1: "21", 2: "22"}
        in_da = {1: "f2", 2: "s0", 3: "s1"}
        before_in_da = {0: "30", 1: "31", 3: "32"}
        earlier_in_hidden = {0: "404142"}
    else:
        in_hidden = {1: "f2", 2: "s0"}
        in_weights = {0: "s1", 1: "s2", 2: "t0"}
        earlier_in_hidden = {0: "t1", 2: "t2"}

    def hidden(t, _):
        for i, what in in_hidden.items():
            when((s > 0) & (t == i), functools.partial(due, before, what))
        for i, what in earlier_in_hidden.items():
            when((s > 1) & (t == i), functools.partial(due, before - 3, what))
        if not with_da:
            when((s == 0) & (t == 3), functools.partial(due, 0, "20"))
            when((s == 1) & (t == 0), functools.partial(due, 0, "31"))
            when((s == 1) & (t == 2), functools.partial(due, 0, "32"))
        rows = chunk(t)
        if with_da:
            a = a_buf[rows, :]
            gate = dot(a, wg_ref[0])
            up = dot(a, wu_ref[0])
        else:
            step = s * steps + t
            for copy in fetch(step):
                copy.wait()
            when(step + 1 < pl.num_programs(0) * steps, lambda: [copy.start() for copy in fetch(step + 1)])
            gate, up = stage[lax.rem(step, 2), 0], stage[lax.rem(step, 2), 1]
        dact = dot_nt(dy_ref[0, rows, :], wd_ref[0]).astype(BF16).astype(F32)
        sig = jax.nn.sigmoid(gate)
        silu = gate * sig
        gu_buf[0, rows, :] = (dact * up * (sig + silu * (1 - sig))).astype(BF16)
        gu_buf[1, rows, :] = (dact * silu).astype(BF16)
        gu_buf[2, rows, :] = (silu * up).astype(BF16)
        return 0

    lax.fori_loop(0, steps, hidden, 0)

    def weights(j, _):
        for i, what in in_weights.items():
            when((s > 0) & (j == i), functools.partial(due, before, what))
        if not with_da:
            when((s == 0) & (j == 1), functools.partial(due, 0, "21"))
            when((s == 0) & (j == 2), functools.partial(due, 0, "2230"))
            when((s == 1) & (j == 0), functools.partial(due, 0, "404142"))
        slot = lax.rem(here + j, depth)
        g_buf[slot] = dot(t_buf[j // 2], gu_buf[j]).astype(BF16)
        ex.swap(here + j, slot).start()
        when(j > 0, lambda: ex.first(here + j - 1, lax.rem(here + j - 1, depth)))
        return 0

    lax.fori_loop(0, 3, weights, 0)

    if with_da:

        def by_a(t, _):
            for i, what in in_da.items():
                when(t == i, functools.partial(due, here, what))
            for i, what in before_in_da.items():
                when((s > 0) & (t == i), functools.partial(due, before, what))
            rows = chunk(t)
            acc[rows, :] += dot_nt(gu_buf[0, rows, :], wg_ref[0]) + dot_nt(gu_buf[1, rows, :], wu_ref[0])
            return 0

        lax.fori_loop(0, steps, by_a, 0)

    @pl.when(s == last)
    def _():
        if with_da:

            def by_h(t, _):
                rows = chunk(t)
                wide = h_ref[0, rows, :].astype(F32)
                scale = norm_scale(wide)
                da = acc[rows, :].astype(BF16).astype(F32)
                through = da * scale - wide * (scale * scale * scale * jnp.mean(da * wide, -1, keepdims=True))
                dh_ref[0, rows, :] = dy_ref[0, rows, :] + through.astype(BF16)
                return 0

            lax.fori_loop(0, steps, by_h, 0)
        if with_da:
            due(before, "404142")
            due(here, "s2t0t1t2")
        else:
            due(before, "t1")
            due(here, "s0f2")
            due(before, "t2")
            due(here, "s1t0s2t1t2")
            squares_over_group(ex, squares_ref, slots, slot_sems)


def backward(n, layer, with_da, h, dy, weights, earlier=()):
    _, tokens, d = h.shape
    ff = weights[0].shape[-1]
    units = 3 * (ff // WIDTH)
    share, chips = d // n, n // 2
    gathered = units - 3 if with_da else 3
    out_shape = [
        jax.ShapeDtypeStruct((8, 128), F32),
        jax.ShapeDtypeStruct((gathered, d, WIDTH), BF16),
    ]
    out_specs = [once(out_shape[0].shape), pl.BlockSpec(memory_space=pl.ANY)]
    if with_da:
        out_shape += [jax.ShapeDtypeStruct((units, share, WIDTH), BF16), jax.ShapeDtypeStruct(h.shape, BF16)]
        more = weight_specs(layer, d)
        scratch = [pltpu.VMEM((tokens, d), BF16), pltpu.VMEM((tokens, d), F32)]
    else:
        out_shape += [jax.ShapeDtypeStruct((units, share // 2, WIDTH), BF16)] * 2
        last = units // 3 - 1
        anywhere = pl.BlockSpec(memory_space=pl.ANY)
        share_spec = pl.BlockSpec((3, share, WIDTH), lambda s: (last, 0, 0), pipeline_mode=pl.Buffered(1))
        more = weight_specs(layer, d)[2:] + [anywhere, anywhere, share_spec, once((8, 128))]
        weights = weights[2:]
        scratch = [pltpu.VMEM((2, 2, CHUNK, WIDTH), F32), pltpu.SemaphoreType.DMA((2, 2))]
    out_specs += [once(o.shape) for o in out_shape[2:]]
    return pl.pallas_call(
        functools.partial(backward_kernel, n, with_da),
        grid=(ff // WIDTH,),
        in_specs=[once(h.shape), once(h.shape)] + more,
        out_specs=out_specs,
        out_shape=out_shape,
        scratch_shapes=scratch
        + [
            pltpu.VMEM((2, d, tokens), BF16),
            pltpu.VMEM((3, tokens, WIDTH), BF16),
            pltpu.VMEM((SLOTS, d, WIDTH), BF16),
            pltpu.VMEM((units, chips * share, WIDTH), BF16),
            pltpu.VMEM((units, 2, share // 2, WIDTH), BF16),
            pltpu.VMEM((units, 2, share, WIDTH), BF16),
            pltpu.VMEM((chips + 2, 8, 128), F32),
            pltpu.SemaphoreType.DMA((2, units)),
            pltpu.SemaphoreType.DMA((2, units, 6)),
            pltpu.SemaphoreType.DMA((2, gathered, 9)),
            pltpu.SemaphoreType.DMA((gathered,)),
            pltpu.SemaphoreType.DMA((2, 4)),
        ],
        compiler_params=pltpu.CompilerParams(
            vmem_limit_bytes=VMEM_LIMIT, dimension_semantics=("arbitrary",), collective_id=1 + layer, has_side_effects=True
        ),
        name=f"backward_{layer}",
    )(h, dy, *weights, *earlier)


def adamw_kernel(count, rows_ref, q_ref, pieces, refs):
    ws, ms, vs = refs[0:3], refs[3:6], refs[6:9]
    new_ws, new_ms, new_vs = refs[9:12], refs[12:15], refs[15:18]
    factor = jnp.minimum(1.0, 0.5 * lax.rsqrt(jnp.full((1, 1), jnp.sum(q_ref[...]) / count, F32) + 1e-30))

    def update(g, w, m, v, new_w, new_m, new_v, rows, columns):
        at = (0, rows, columns)
        g = g * factor
        m = 0.9 * m[at] + 0.1 * g
        v = 0.95 * v[at] + 0.05 * g * g
        new_m[at] = m
        new_v[at] = v
        wide = w[at].astype(F32)
        new_w[at] = (wide - 0.02 * (m * lax.rsqrt(v + 1e-8) + 0.1 * wide)).astype(BF16)

    everything = list(zip(ws, ms, vs, new_ws, new_ms, new_vs, strict=True))
    g_ref = pieces[0]
    if len(pieces) > 1:
        g_ref = refs[18]
        for i, piece in enumerate(pieces):
            size = piece.shape[1]
            for j in range(3):
                g_ref[j, pl.ds(pl.multiple_of(rows_ref[i], size), size), :] = piece[j]
    d = g_ref.shape[1]
    for j in range(2):
        for row in range(0, d, 192):
            rows = slice(row, row + 192)
            update(g_ref[j, rows, :].astype(F32), *everything[j], rows, slice(None))
    for row in range(0, d, 384):
        rows = slice(row, row + 384)
        update(g_ref[2, rows, :].astype(F32).T, *everything[2], slice(None), rows)


def adamw(squares, layer, slices, pieces, rows, weights, m, v, earlier):
    layers, d, ff = weights[0].shape
    strips = WIDTH // STRIP
    start = slices[0] * strips
    wide = pl.BlockSpec((1, d, STRIP), lambda s: (layer, 0, start + s))
    tall = pl.BlockSpec((1, STRIP, d), lambda s: (layer, start + s, 0))
    three = [wide, wide, tall]
    anywhere = [pl.BlockSpec(memory_space=pl.ANY)] * len(earlier)
    count = sum(w.size for w in weights)
    k, parts = len(pieces), slices[1] - slices[0]

    def kernel(rows_ref, q_ref, *refs):
        refs = refs[: k + 9] + refs[k + 9 + len(earlier) :]
        adamw_kernel(count, rows_ref, q_ref, refs[:k], refs[k:])

    return pl.pallas_call(
        kernel,
        grid=(parts * strips,),
        in_specs=[pl.BlockSpec(memory_space=pltpu.SMEM), once((8, 128))]
        + [pl.BlockSpec((3, g.shape[1], STRIP), lambda s: (s // strips, 0, s % strips)) for g in pieces]
        + three * 3
        + anywhere,
        out_specs=three * 3,
        out_shape=[jax.ShapeDtypeStruct(w.shape, t) for t in (BF16, F32, F32) for w in weights],
        scratch_shapes=[pltpu.VMEM((3, d, STRIP), BF16)] if k > 1 else [],
        input_output_aliases={11 + k + i: i for i in range(len(earlier))},
        compiler_params=pltpu.CompilerParams(vmem_limit_bytes=VMEM_LIMIT, dimension_semantics=("arbitrary",)),
        cost_estimate=pl.CostEstimate(flops=10**11 // 6 * parts, bytes_accessed=39 * 10**6 * parts, transcendentals=0),
        name=f"adamw_{layer}_{slices[0]}",
    )(rows, squares, *pieces, *weights, *m, *v, *earlier)


def gathered(n, own, first, second):
    chips, half = n // 2, own[0].shape[1]
    share = 2 * half
    me = lax.axis_index("dp")
    core, chip = me % 2, me // 2
    left, right, far = (chip + chips - 1) % chips, (chip + 1) % chips, (chip + 2) % chips

    def shift(a, by):
        return lax.ppermute(a, "dp", [(c * 2 + k, (c + by) % chips * 2 + k) for c in range(chips) for k in range(2)])

    def swap(a):
        return lax.ppermute(a, "dp", [(i, i ^ 1) for i in range(n)])

    top, bottom = own
    from_left = [shift(top, 1), shift(bottom, 1)]
    from_right = [shift(bottom, -1), shift(top, -1)]
    result = first()
    from_left, from_right, result = lax.optimization_barrier((from_left, from_right, result))
    far_top, far_bottom = shift(from_left[0], 1), shift(from_right[0], -1)
    near = [top, bottom, *from_left, *from_right]
    near_there = [swap(piece) for piece in near]
    result = second(result)
    far_top, far_bottom, result = lax.optimization_barrier((far_top, far_bottom, result))
    pieces = near + [far_top, far_bottom] + near_there + [swap(far_top), swap(far_bottom)]
    rows = [chip * share, chip * share + half, left * share, left * share + half, right * share + half, right * share, far * share, far * share + half]
    rows = [core * chips * share + row for row in rows] + [(1 - core) * chips * share + row for row in rows]
    return pieces, jnp.stack(rows).astype(jnp.int32), result


def solution(mesh):
    n = mesh.shape["dp"]

    def step(x, dy, *arrays):
        weights, m, v = (arrays[i : i + 3] for i in (0, 3, 6))
        slices = weights[0].shape[-1] // WIDTH
        h, gate, up = forward(0, x, weights)
        squares, g_1, own_1, dh = backward(n, 1, True, h, dy, weights)
        squares, g_1_last, *own_0 = backward(n, 0, False, x, dh, weights, (gate, up, own_1, squares))
        nowhere = jnp.zeros((1,), jnp.int32)
        pieces, rows, new = gathered(
            n,
            own_0,
            lambda: adamw(squares, 1, (0, slices - 1), [g_1], nowhere, weights, m, v, ()),
            lambda new: adamw(squares, 1, (slices - 1, slices), [g_1_last], nowhere, weights, m, v, new),
        )
        return tuple(adamw(squares, 0, (0, slices), pieces, rows, weights, m, v, new))

    return jax.shard_map(
        step,
        mesh=mesh,
        in_specs=(P(("rep", "dp"), None, None),) * 2 + (P(None, None, None),) * 9,
        out_specs=(P("rep", None, None),) * 9,
        check_vma=False,
    )
```

```python
import functools

import jax
import jax.numpy as jnp
from jax import lax
from jax.experimental import pallas as pl
from jax.experimental.pallas import tpu as pltpu
from jax.sharding import PartitionSpec as P

F32, BF16 = jnp.float32, jnp.bfloat16
MESH = pl.DeviceIdType.MESH
WIDTH = 768
STRIP = 384
CHUNK = 512
SLOTS = 6
VMEM_LIMIT = 63 * 1024 * 1024
NT = (((1,), (1,)), ((), ()))


def dot(a, b):
    return jnp.dot(a, b, preferred_element_type=F32)


def dot_nt(a, b):
    return lax.dot_general(a, b, NT, preferred_element_type=F32)


def norm_scale(wide):
    return lax.rsqrt(jnp.mean(wide**2, -1, keepdims=True) + 1e-6)


def normed(h):
    wide = h.astype(F32)
    return (wide * norm_scale(wide)).astype(BF16)


def once(shape):
    return pl.BlockSpec(shape, lambda *_: (0,) * len(shape), pipeline_mode=pl.Buffered(1))


def forward_kernel(h_ref, wg_ref, wu_ref, wd_ref, out_ref, gate_hbm, up_hbm, a_buf, acc, stage, sems):
    s = pl.program_id(0)
    tokens = a_buf.shape[0]
    steps = tokens // CHUNK
    count = pl.num_programs(0) * steps

    def chunk(t):
        return pl.ds(pl.multiple_of(t * CHUNK, CHUNK), CHUNK)

    def keep(step):
        slot = lax.rem(step, 2)
        return [pltpu.make_async_copy(stage.at[slot, i], to.at[step // steps, chunk(lax.rem(step, steps))], sems.at[slot, i]) for i, to in enumerate((gate_hbm, up_hbm))]

    @pl.when(s == 0)
    def _():
        def prepare(t, _):
            rows = chunk(t)
            a_buf[rows, :] = normed(h_ref[0, rows, :])
            acc[rows, :] = jnp.zeros((CHUNK, acc.shape[1]), F32)
            return 0

        lax.fori_loop(0, steps, prepare, 0)

    def hidden(t, _):
        rows, step = chunk(t), s * steps + t
        slot = lax.rem(step, 2)

        @pl.when(step >= 2)
        def _():
            for copy in keep(step - 2):
                copy.wait()

        a = a_buf[rows, :]
        gate = dot(a, wg_ref[0])
        up = dot(a, wu_ref[0])
        stage[slot, 0] = gate
        stage[slot, 1] = up
        for copy in keep(step):
            copy.start()
        act = (gate * jax.nn.sigmoid(gate) * up).astype(BF16)
        acc[rows, :] += dot(act, wd_ref[0])
        return 0

    lax.fori_loop(0, steps, hidden, 0)

    @pl.when(s == pl.num_programs(0) - 1)
    def _():
        def finish(t, _):
            rows = chunk(t)
            out_ref[0, rows, :] = h_ref[0, rows, :] + acc[rows, :].astype(BF16)
            return 0

        lax.fori_loop(0, steps, finish, 0)
        for step in (count - 2, count - 1):
            for copy in keep(step):
                copy.wait()


def weight_specs(layer, d):
    wide = pl.BlockSpec((1, d, WIDTH), lambda s: (layer, 0, s))
    return [wide, wide, pl.BlockSpec((1, WIDTH, d), lambda s: (layer, s, 0))]


def forward(layer, h, weights):
    _, tokens, d = h.shape
    ff = weights[0].shape[-1]
    kept = jax.ShapeDtypeStruct((ff // WIDTH, tokens, WIDTH), F32)
    return pl.pallas_call(
        forward_kernel,
        grid=(ff // WIDTH,),
        in_specs=[once(h.shape)] + weight_specs(layer, d),
        out_specs=[once(h.shape), pl.BlockSpec(memory_space=pl.ANY), pl.BlockSpec(memory_space=pl.ANY)],
        out_shape=[jax.ShapeDtypeStruct(h.shape, BF16), kept, kept],
        scratch_shapes=[
            pltpu.VMEM((tokens, d), BF16),
            pltpu.VMEM((tokens, d), F32),
            pltpu.VMEM((2, 2, CHUNK, WIDTH), F32),
            pltpu.SemaphoreType.DMA((2, 2)),
        ],
        compiler_params=pltpu.CompilerParams(vmem_limit_bytes=VMEM_LIMIT, dimension_semantics=("arbitrary",)),
        name="forward",
    )(h, *weights)


class Exchange:
    def __init__(self, n, g_buf, got_half, got_far, got_near, own_refs, squares, sems):
        self.g_buf, self.got_half, self.got_far, self.got_near = g_buf, got_half, got_far, got_near
        self.own_refs, self.squares = own_refs, squares
        self.swap_sems, self.sems = sems
        me = lax.axis_index("dp")
        self.core, self.chip = lax.rem(me, 2), me // 2
        self.chips = n // 2
        self.right = lax.rem(self.chip + 1, self.chips)
        self.left = lax.rem(self.chip + self.chips - 1, self.chips)
        self.far = lax.rem(self.chip + 2, self.chips)
        self.row = (self.core * self.chips + self.chip) * got_near.shape[2]
        self.share = got_near.shape[2]

    def to(self, chip, core):
        return {"dp": chip * 2 + core}

    def barrier(self, far):
        barrier = pltpu.get_barrier_semaphore()
        peers = [(self.chip, 1 - self.core), (self.right, self.core), (self.left, self.core)]
        if far:
            peers.append((self.far, self.core))
            peers += [(chip, 1 - self.core) for chip in (self.right, self.left, self.far)]
        for peer in peers:
            pl.semaphore_signal(barrier, inc=1, device_id=self.to(*peer), device_id_type=MESH)
        pl.semaphore_wait(barrier, len(peers))

    def swap(self, u, slot):
        rows = self.share * self.chips
        other = pl.ds(pl.multiple_of((1 - self.core) * rows, rows), rows)
        return pltpu.make_async_remote_copy(
            src_ref=self.g_buf.at[slot, other],
            dst_ref=self.got_half.at[u],
            send_sem=self.swap_sems.at[0, u],
            recv_sem=self.swap_sems.at[1, u],
            device_id=self.to(self.chip, 1 - self.core),
            device_id_type=MESH,
        )

    def at(self, slot, chip, top=True, bottom=True):
        start = (self.core * self.chips + chip) * self.share + (0 if top else self.share // 2)
        size = self.share if top and bottom else self.share // 2
        return self.g_buf.at[slot, pl.ds(pl.multiple_of(start, size), size)]

    def copy(self, u, slot, which):
        top, bottom = pl.ds(0, self.share // 2), pl.ds(self.share // 2, self.share // 2)
        source, target, chip = {
            0: (self.at(slot, self.far, bottom=False), self.got_far.at[u, 0], self.right),
            1: (self.at(slot, self.far, top=False), self.got_far.at[u, 1], self.left),
            2: (self.at(slot, self.right, top=False), self.got_near.at[u, 0, bottom], self.right),
            3: (self.at(slot, self.left, bottom=False), self.got_near.at[u, 1, top], self.left),
            4: (self.at(slot, self.right, bottom=False), self.got_near.at[u, 0, top], self.right),
            5: (self.at(slot, self.left, top=False), self.got_near.at[u, 1, bottom], self.left),
        }[which]
        return pltpu.make_async_remote_copy(
            src_ref=source,
            dst_ref=target,
            send_sem=self.sems.at[0, u, which],
            recv_sem=self.sems.at[1, u, which],
            device_id=self.to(chip, self.core),
            device_id_type=MESH,
        )

    def first(self, u, slot):
        self.swap(u, slot).wait()
        for chip in range(self.chips):
            there = pl.ds(chip * self.share, self.share)
            mine = self.at(slot, chip)
            mine[...] = (mine[...].astype(F32) + self.got_half[u, there, :].astype(F32)).astype(BF16)
        for which in range(4):
            self.copy(u, slot, which).start()

    def second(self, u, slot):
        for which, mine in ((0, self.at(slot, self.right, bottom=False)), (1, self.at(slot, self.left, top=False))):
            self.copy(u, slot, which).wait_recv()
            mine[...] = (mine[...].astype(F32) + self.got_far[u, which].astype(F32)).astype(BF16)
            self.copy(u, slot, which + 4).start()

    def third(self, u, slot):
        for which in range(2, 6):
            self.copy(u, slot, which).wait_recv()
        total = self.at(slot, self.chip)[...].astype(F32) + self.got_near[u, 0].astype(F32) + self.got_near[u, 1].astype(F32)
        total = total.astype(BF16)
        if len(self.own_refs) == 1:
            self.own_refs[0][u] = total
        else:
            for part, half in zip(self.own_refs, (total[: self.share // 2], total[self.share // 2 :]), strict=True):
                part[u] = half
        wide = total.astype(F32)
        wide = (wide * wide).reshape(-1, 8, wide.shape[-1]).sum(0)
        self.squares[...] += sum(wide[:, i : i + 128] for i in range(0, wide.shape[-1], 128))
        for which in range(6):
            self.copy(u, slot, which).wait_send()


class Gather:
    def __init__(self, ex, own_ref, first, g_ref, sems, local_sem):
        self.ex, self.own_ref, self.first, self.g_ref, self.sems, self.local_sem = ex, own_ref, first, g_ref, sems, local_sem

    def rows(self, u, chip, top=True, bottom=True):
        ex = self.ex
        start = (ex.core * ex.chips + chip) * ex.share + (0 if top else ex.share // 2)
        size = ex.share if top and bottom else ex.share // 2
        return self.g_ref.at[u, pl.ds(pl.multiple_of(start, size), size)]

    def copy(self, u, which):
        ex = self.ex
        here = (ex.chip, 1 - ex.core)
        mine = self.rows(u, ex.chip)
        source, target, to = {
            0: (self.own_ref.at[self.first + u], mine, (ex.right, ex.core)),
            1: (self.own_ref.at[self.first + u], mine, (ex.left, ex.core)),
            2: (self.own_ref.at[self.first + u], mine, here),
            3: (self.rows(u, ex.left, bottom=False),) * 2 + ((ex.right, ex.core),),
            4: (self.rows(u, ex.right, top=False),) * 2 + ((ex.left, ex.core),),
            5: (self.rows(u, ex.left),) * 2 + (here,),
            6: (self.rows(u, ex.right),) * 2 + (here,),
            7: (self.rows(u, ex.far, bottom=False),) * 2 + (here,),
            8: (self.rows(u, ex.far, top=False),) * 2 + (here,),
        }[which]
        return pltpu.make_async_remote_copy(
            src_ref=source,
            dst_ref=target,
            send_sem=self.sems.at[0, u, which],
            recv_sem=self.sems.at[1, u, which],
            device_id=ex.to(*to),
            device_id_type=MESH,
        )

    def local(self, u):
        return pltpu.make_async_copy(self.own_ref.at[self.first + u], self.rows(u, self.ex.chip), self.local_sem.at[u])

    def one(self, u):
        for which in range(3):
            self.copy(u, which).start()
        self.local(u).start()

    def two(self, u):
        for which in range(2):
            self.copy(u, which).wait_recv()
            self.copy(u, which + 3).start()
            self.copy(u, which + 5).start()

    def three(self, u):
        for which in range(2):
            self.copy(u, which + 3).wait_recv()
            self.copy(u, which + 7).start()

    def four(self, u):
        for which in (2, 5, 6, 7, 8):
            self.copy(u, which).wait_recv()
        for which in range(9):
            self.copy(u, which).wait_send()
        self.local(u).wait()


def squares_over_group(ex, squares_ref, slots, sems):
    me = ex.chip * 2 + ex.core
    n = 2 * ex.chips

    def send(i):
        return pltpu.make_async_remote_copy(
            src_ref=squares_ref,
            dst_ref=slots.at[me],
            send_sem=sems.at[0, i],
            recv_sem=sems.at[1, i],
            device_id={"dp": lax.rem(me + i, n)},
            device_id_type=MESH,
        )

    copies = [send(i) for i in range(1, n)]
    for copy in copies:
        copy.start()
    slots[me] = squares_ref[...]
    for copy in copies:
        copy.wait()
    total = slots[0]
    for i in range(1, n):
        total = total + slots[i]
    squares_ref[...] = total


def backward_kernel(n, with_da, h_ref, dy_ref, *refs):
    if with_da:
        wg_ref, wu_ref, wd_ref, squares_ref, gathered_ref, own_ref, dh_ref, a_buf, acc, *refs = refs
        own_refs = (own_ref,)
    else:
        wd_ref, gate_hbm, up_hbm, earlier_own_ref, earlier_squares_ref, squares_ref, gathered_ref, *own_refs, stage, stage_sems = refs[:11]
        refs = refs[11:]
    t_buf, gu_buf, g_buf, got_half, got_far, got_near, slots, *sems = refs
    swap_sems, copy_sems, gather_sems, local_sems, slot_sems = sems
    depth = g_buf.shape[0]
    s = pl.program_id(0)
    last = pl.num_programs(0) - 1
    _, tokens, d = h_ref.shape
    steps = tokens // CHUNK
    ex = Exchange(n, g_buf, got_half, got_far, got_near, own_refs, squares_ref, (swap_sems, copy_sems))
    gather = Gather(ex, own_ref if with_da else earlier_own_ref, 0, gathered_ref, gather_sems, local_sems)

    def chunk(t):
        return pl.ds(pl.multiple_of(t * CHUNK, CHUNK), CHUNK)

    def each(f, start=0):
        lax.fori_loop(0, 3, lambda j, _: (f(start + j), 0)[1], 0)

    def fetch(step):
        slot = lax.rem(step, 2)
        return [pltpu.make_async_copy(kept.at[step // steps, chunk(lax.rem(step, steps))], stage.at[slot, i], stage_sems.at[slot, i]) for i, kept in enumerate((gate_hbm, up_hbm))]

    @pl.when(s == 0)
    def _():
        if not with_da:
            for copy in fetch(0):
                copy.start()
        ex.barrier(not with_da)
        if with_da:
            squares_ref[...] = jnp.zeros_like(squares_ref)
        else:
            squares_ref[...] = earlier_squares_ref[...]
            each(gather.one)

        def prepare(t, _):
            rows = chunk(t)
            a = normed(h_ref[0, rows, :])
            t_buf[0, :, rows] = a.T
            t_buf[1, :, rows] = dy_ref[0, rows, :].T
            if with_da:
                a_buf[rows, :] = a
                acc[rows, :] = jnp.zeros((CHUNK, d), F32)
            return 0

        lax.fori_loop(0, steps, prepare, 0)

    def due(u, what):
        steps = {"f": ex.first, "s": ex.second, "t": ex.third}
        gathers = {"1": gather.one, "2": gather.two, "3": gather.three, "4": gather.four}
        for step, j in zip(what[::2], map(int, what[1::2])):
            if step in steps:
                steps[step](u + j, lax.rem(u + j, depth))
            else:
                gathers[step](u + j)

    here, before = 3 * s, 3 * (s - 1)

    def when(condition, *actions):
        @pl.when(condition)
        def _():
            for action in actions:
                action()

    if with_da:
        in_hidden = {1: "s2", 2: "t010t111", 3: "t212"}
        in_weights = {0: "20", 1: "21", 2: "22"}
        in_da = {1: "f2", 2: "s0", 3: "s1"}
        before_in_da = {0: "30", 1: "31", 3: "32"}
        earlier_in_hidden = {0: "404142"}
    else:
        in_hidden = {1: "f2", 2: "s0"}
        in_weights = {0: "s1", 1: "s2", 2: "t0"}
        earlier_in_hidden = {0: "t1", 2: "t2"}

    def hidden(t, _):
        for i, what in in_hidden.items():
            when((s > 0) & (t == i), functools.partial(due, before, what))
        for i, what in earlier_in_hidden.items():
            when((s > 1) & (t == i), functools.partial(due, before - 3, what))
        if not with_da:
            when((s == 0) & (t == 3), functools.partial(due, 0, "20"))
            when((s == 1) & (t == 0), functools.partial(due, 0, "31"))
            when((s == 1) & (t == 2), functools.partial(due, 0, "32"))
        rows = chunk(t)
        if with_da:
            a = a_buf[rows, :]
            gate = dot(a, wg_ref[0])
            up = dot(a, wu_ref[0])
        else:
            step = s * steps + t
            for copy in fetch(step):
                copy.wait()
            when(step + 1 < pl.num_programs(0) * steps, lambda: [copy.start() for copy in fetch(step + 1)])
            gate, up = stage[lax.rem(step, 2), 0], stage[lax.rem(step, 2), 1]
        dact = dot_nt(dy_ref[0, rows, :], wd_ref[0]).astype(BF16).astype(F32)
        sig = jax.nn.sigmoid(gate)
        silu = gate * sig
        gu_buf[0, rows, :] = (dact * up * (sig + silu * (1 - sig))).astype(BF16)
        gu_buf[1, rows, :] = (dact * silu).astype(BF16)
        gu_buf[2, rows, :] = (silu * up).astype(BF16)
        return 0

    lax.fori_loop(0, steps, hidden, 0)

    def weights(j, _):
        for i, what in in_weights.items():
            when((s > 0) & (j == i), functools.partial(due, before, what))
        if not with_da:
            when((s == 0) & (j == 1), functools.partial(due, 0, "21"))
            when((s == 0) & (j == 2), functools.partial(due, 0, "2230"))
            when((s == 1) & (j == 0), functools.partial(due, 0, "404142"))
        slot = lax.rem(here + j, depth)
        g_buf[slot] = dot(t_buf[j // 2], gu_buf[j]).astype(BF16)
        ex.swap(here + j, slot).start()
        when(j > 0, lambda: ex.first(here + j - 1, lax.rem(here + j - 1, depth)))
        return 0

    lax.fori_loop(0, 3, weights, 0)

    if with_da:

        def by_a(t, _):
            for i, what in in_da.items():
                when(t == i, functools.partial(due, here, what))
            for i, what in before_in_da.items():
                when((s > 0) & (t == i), functools.partial(due, before, what))
            rows = chunk(t)
            acc[rows, :] += dot_nt(gu_buf[0, rows, :], wg_ref[0]) + dot_nt(gu_buf[1, rows, :], wu_ref[0])
            return 0

        lax.fori_loop(0, steps, by_a, 0)

    @pl.when(s == last)
    def _():
        if with_da:

            def by_h(t, _):
                rows = chunk(t)
                wide = h_ref[0, rows, :].astype(F32)
                scale = norm_scale(wide)
                da = acc[rows, :].astype(BF16).astype(F32)
                through = da * scale - wide * (scale * scale * scale * jnp.mean(da * wide, -1, keepdims=True))
                dh_ref[0, rows, :] = dy_ref[0, rows, :] + through.astype(BF16)
                return 0

            lax.fori_loop(0, steps // 2, by_h, 0)
            due(here, "s2t0")
            lax.fori_loop(steps // 2, steps, by_h, 0)
            due(before, "404142")
            due(here, "t1t2")
        else:
            due(before, "t1")
            due(here, "s0f2")
            due(before, "t2")
            due(here, "s1t0s2t1t2")
            squares_over_group(ex, squares_ref, slots, slot_sems)


def backward(n, layer, with_da, h, dy, weights, earlier=()):
    _, tokens, d = h.shape
    ff = weights[0].shape[-1]
    units = 3 * (ff // WIDTH)
    share, chips = d // n, n // 2
    gathered = units - 3 if with_da else 3
    out_shape = [
        jax.ShapeDtypeStruct((8, 128), F32),
        jax.ShapeDtypeStruct((gathered, d, WIDTH), BF16),
    ]
    out_specs = [once(out_shape[0].shape), pl.BlockSpec(memory_space=pl.ANY)]
    if with_da:
        out_shape += [jax.ShapeDtypeStruct((units, share, WIDTH), BF16), jax.ShapeDtypeStruct(h.shape, BF16)]
        more = weight_specs(layer, d)
        scratch = [pltpu.VMEM((tokens, d), BF16), pltpu.VMEM((tokens, d), F32)]
    else:
        out_shape += [jax.ShapeDtypeStruct((units, share // 2, WIDTH), BF16)] * 2
        last = units // 3 - 1
        anywhere = pl.BlockSpec(memory_space=pl.ANY)
        share_spec = pl.BlockSpec((3, share, WIDTH), lambda s: (last, 0, 0), pipeline_mode=pl.Buffered(1))
        more = weight_specs(layer, d)[2:] + [anywhere, anywhere, share_spec, once((8, 128))]
        weights = weights[2:]
        scratch = [pltpu.VMEM((2, 2, CHUNK, WIDTH), F32), pltpu.SemaphoreType.DMA((2, 2))]
    out_specs += [once(o.shape) for o in out_shape[2:]]
    return pl.pallas_call(
        functools.partial(backward_kernel, n, with_da),
        grid=(ff // WIDTH,),
        in_specs=[once(h.shape), once(h.shape)] + more,
        out_specs=out_specs,
        out_shape=out_shape,
        scratch_shapes=scratch
        + [
            pltpu.VMEM((2, d, tokens), BF16),
            pltpu.VMEM((3, tokens, WIDTH), BF16),
            pltpu.VMEM((SLOTS, d, WIDTH), BF16),
            pltpu.VMEM((units, chips * share, WIDTH), BF16),
            pltpu.VMEM((units, 2, share // 2, WIDTH), BF16),
            pltpu.VMEM((units, 2, share, WIDTH), BF16),
            pltpu.VMEM((n, 8, 128), F32),
            pltpu.SemaphoreType.DMA((2, units)),
            pltpu.SemaphoreType.DMA((2, units, 6)),
            pltpu.SemaphoreType.DMA((2, gathered, 9)),
            pltpu.SemaphoreType.DMA((gathered,)),
            pltpu.SemaphoreType.DMA((2, n)),
        ],
        compiler_params=pltpu.CompilerParams(
            vmem_limit_bytes=VMEM_LIMIT, dimension_semantics=("arbitrary",), collective_id=1 + layer, has_side_effects=True
        ),
        name=f"backward_{layer}",
    )(h, dy, *weights, *earlier)


def adamw_kernel(count, rows_ref, q_ref, pieces, refs):
    ws, ms, vs = refs[0:3], refs[3:6], refs[6:9]
    new_ws, new_ms, new_vs = refs[9:12], refs[12:15], refs[15:18]
    factor = jnp.minimum(1.0, 0.5 * lax.rsqrt(jnp.full((1, 1), jnp.sum(q_ref[...]) / count, F32) + 1e-30))

    def update(g, w, m, v, new_w, new_m, new_v, rows, columns):
        at = (0, rows, columns)
        g = g * factor
        m = 0.9 * m[at] + 0.1 * g
        v = 0.95 * v[at] + 0.05 * g * g
        new_m[at] = m
        new_v[at] = v
        wide = w[at].astype(F32)
        new_w[at] = (wide - 0.02 * (m * lax.rsqrt(v + 1e-8) + 0.1 * wide)).astype(BF16)

    everything = list(zip(ws, ms, vs, new_ws, new_ms, new_vs, strict=True))
    g_ref = pieces[0]
    if len(pieces) > 1:
        g_ref = refs[18]
        for i, piece in enumerate(pieces):
            size = piece.shape[1]
            for j in range(3):
                g_ref[j, pl.ds(pl.multiple_of(rows_ref[i], size), size), :] = piece[j]
    d = g_ref.shape[1]
    for j in range(2):
        for row in range(0, d, 192):
            rows = slice(row, row + 192)
            update(g_ref[j, rows, :].astype(F32), *everything[j], rows, slice(None))
    for row in range(0, d, 384):
        rows = slice(row, row + 384)
        update(g_ref[2, rows, :].astype(F32).T, *everything[2], slice(None), rows)


def adamw(squares, layer, slices, pieces, rows, weights, m, v, earlier):
    layers, d, ff = weights[0].shape
    strips = WIDTH // STRIP
    start = slices[0] * strips
    wide = pl.BlockSpec((1, d, STRIP), lambda s: (layer, 0, start + s))
    tall = pl.BlockSpec((1, STRIP, d), lambda s: (layer, start + s, 0))
    three = [wide, wide, tall]
    anywhere = [pl.BlockSpec(memory_space=pl.ANY)] * len(earlier)
    count = sum(w.size for w in weights)
    k, parts = len(pieces), slices[1] - slices[0]

    def kernel(rows_ref, q_ref, *refs):
        refs = refs[: k + 9] + refs[k + 9 + len(earlier) :]
        adamw_kernel(count, rows_ref, q_ref, refs[:k], refs[k:])

    return pl.pallas_call(
        kernel,
        grid=(parts * strips,),
        in_specs=[pl.BlockSpec(memory_space=pltpu.SMEM), once((8, 128))]
        + [pl.BlockSpec((3, g.shape[1], STRIP), lambda s: (s // strips, 0, s % strips)) for g in pieces]
        + three * 3
        + anywhere,
        out_specs=three * 3,
        out_shape=[jax.ShapeDtypeStruct(w.shape, t) for t in (BF16, F32, F32) for w in weights],
        scratch_shapes=[pltpu.VMEM((3, d, STRIP), BF16)] if k > 1 else [],
        input_output_aliases={11 + k + i: i for i in range(len(earlier))},
        compiler_params=pltpu.CompilerParams(vmem_limit_bytes=VMEM_LIMIT, dimension_semantics=("arbitrary",)),
        cost_estimate=pl.CostEstimate(flops=10**11 // 6 * parts, bytes_accessed=39 * 10**6 * parts, transcendentals=0),
        name=f"adamw_{layer}_{slices[0]}",
    )(rows, squares, *pieces, *weights, *m, *v, *earlier)


def gathered(n, own, first, second):
    chips, half = n // 2, own[0].shape[1]
    share = 2 * half
    me = lax.axis_index("dp")
    core, chip = me % 2, me // 2
    left, right, far = (chip + chips - 1) % chips, (chip + 1) % chips, (chip + 2) % chips

    def shift(a, by):
        return lax.ppermute(a, "dp", [(c * 2 + k, (c + by) % chips * 2 + k) for c in range(chips) for k in range(2)])

    def swap(a):
        return lax.ppermute(a, "dp", [(i, i ^ 1) for i in range(n)])

    top, bottom = own
    from_left = [shift(top, 1), shift(bottom, 1)]
    from_right = [shift(bottom, -1), shift(top, -1)]
    result = first()
    from_left, from_right, result = lax.optimization_barrier((from_left, from_right, result))
    far_top, far_bottom = shift(from_left[0], 1), shift(from_right[0], -1)
    near = [top, bottom, *from_left, *from_right]
    near_there = [swap(piece) for piece in near]
    result = second(result)
    far_top, far_bottom, result = lax.optimization_barrier((far_top, far_bottom, result))
    pieces = near + [far_top, far_bottom] + near_there + [swap(far_top), swap(far_bottom)]
    rows = [chip * share, chip * share + half, left * share, left * share + half, right * share + half, right * share, far * share, far * share + half]
    rows = [core * chips * share + row for row in rows] + [(1 - core) * chips * share + row for row in rows]
    return pieces, jnp.stack(rows).astype(jnp.int32), result


def solution(mesh):
    n = mesh.shape["dp"]

    def step(x, dy, *arrays):
        weights, m, v = (arrays[i : i + 3] for i in (0, 3, 6))
        slices = weights[0].shape[-1] // WIDTH
        h, gate, up = forward(0, x, weights)
        squares, g_1, own_1, dh = backward(n, 1, True, h, dy, weights)
        squares, g_1_last, *own_0 = backward(n, 0, False, x, dh, weights, (gate, up, own_1, squares))
        nowhere = jnp.zeros((1,), jnp.int32)
        pieces, rows, new = gathered(
            n,
            own_0,
            lambda: adamw(squares, 1, (0, slices - 1), [g_1], nowhere, weights, m, v, ()),
            lambda new: adamw(squares, 1, (slices - 1, slices), [g_1_last], nowhere, weights, m, v, new),
        )
        return tuple(adamw(squares, 0, (0, slices), pieces, rows, weights, m, v, new))

    return jax.shard_map(
        step,
        mesh=mesh,
        in_specs=(P(("rep", "dp"), None, None),) * 2 + (P(None, None, None),) * 9,
        out_specs=(P("rep", None, None),) * 9,
        check_vma=False,
    )
```

```python
import functools

import jax
import jax.numpy as jnp
from jax import lax
from jax.experimental import pallas as pl
from jax.experimental.pallas import tpu as pltpu
from jax.sharding import PartitionSpec as P

F32, BF16 = jnp.float32, jnp.bfloat16
MESH = pl.DeviceIdType.MESH
WIDTH = 768
STRIP = 384
CHUNK = 512
SLOTS = 6
VMEM_LIMIT = 63 * 1024 * 1024
NT = (((1,), (1,)), ((), ()))


def dot(a, b):
    return jnp.dot(a, b, preferred_element_type=F32)


def dot_nt(a, b):
    return lax.dot_general(a, b, NT, preferred_element_type=F32)


def norm_scale(wide):
    return lax.rsqrt(jnp.mean(wide**2, -1, keepdims=True) + 1e-6)


def normed(h):
    wide = h.astype(F32)
    return (wide * norm_scale(wide)).astype(BF16)


def once(shape):
    return pl.BlockSpec(shape, lambda *_: (0,) * len(shape), pipeline_mode=pl.Buffered(1))


def forward_kernel(h_ref, wg_ref, wu_ref, wd_ref, out_ref, gate_hbm, up_hbm, a_buf, acc, stage, sems):
    s = pl.program_id(0)
    tokens = a_buf.shape[0]
    steps = tokens // CHUNK
    count = pl.num_programs(0) * steps

    def chunk(t):
        return pl.ds(pl.multiple_of(t * CHUNK, CHUNK), CHUNK)

    def keep(step):
        slot = lax.rem(step, 2)
        return [pltpu.make_async_copy(stage.at[slot, i], to.at[step // steps, chunk(lax.rem(step, steps))], sems.at[slot, i]) for i, to in enumerate((gate_hbm, up_hbm))]

    @pl.when(s == 0)
    def _():
        def prepare(t, _):
            rows = chunk(t)
            a_buf[rows, :] = normed(h_ref[0, rows, :])
            acc[rows, :] = jnp.zeros((CHUNK, acc.shape[1]), F32)
            return 0

        lax.fori_loop(0, steps, prepare, 0)

    def hidden(t, _):
        rows, step = chunk(t), s * steps + t
        slot = lax.rem(step, 2)

        @pl.when(step >= 2)
        def _():
            for copy in keep(step - 2):
                copy.wait()

        a = a_buf[rows, :]
        gate = dot(a, wg_ref[0])
        up = dot(a, wu_ref[0])
        stage[slot, 0] = gate
        stage[slot, 1] = up
        for copy in keep(step):
            copy.start()
        act = (gate * jax.nn.sigmoid(gate) * up).astype(BF16)
        acc[rows, :] += dot(act, wd_ref[0])
        return 0

    lax.fori_loop(0, steps, hidden, 0)

    @pl.when(s == pl.num_programs(0) - 1)
    def _():
        def finish(t, _):
            rows = chunk(t)
            out_ref[0, rows, :] = h_ref[0, rows, :] + acc[rows, :].astype(BF16)
            return 0

        lax.fori_loop(0, steps, finish, 0)
        for step in (count - 2, count - 1):
            for copy in keep(step):
                copy.wait()


def weight_specs(layer, d):
    wide = pl.BlockSpec((1, d, WIDTH), lambda s: (layer, 0, s))
    return [wide, wide, pl.BlockSpec((1, WIDTH, d), lambda s: (layer, s, 0))]


def forward(layer, h, weights):
    _, tokens, d = h.shape
    ff = weights[0].shape[-1]
    kept = jax.ShapeDtypeStruct((ff // WIDTH, tokens, WIDTH), F32)
    return pl.pallas_call(
        forward_kernel,
        grid=(ff // WIDTH,),
        in_specs=[once(h.shape)] + weight_specs(layer, d),
        out_specs=[once(h.shape), pl.BlockSpec(memory_space=pl.ANY), pl.BlockSpec(memory_space=pl.ANY)],
        out_shape=[jax.ShapeDtypeStruct(h.shape, BF16), kept, kept],
        scratch_shapes=[
            pltpu.VMEM((tokens, d), BF16),
            pltpu.VMEM((tokens, d), F32),
            pltpu.VMEM((2, 2, CHUNK, WIDTH), F32),
            pltpu.SemaphoreType.DMA((2, 2)),
        ],
        compiler_params=pltpu.CompilerParams(vmem_limit_bytes=VMEM_LIMIT, dimension_semantics=("arbitrary",)),
        name="forward",
    )(h, *weights)


class Exchange:
    def __init__(self, n, g_buf, got_half, got_far, got_near, own_refs, squares, sems):
        self.g_buf, self.got_half, self.got_far, self.got_near = g_buf, got_half, got_far, got_near
        self.own_refs, self.squares = own_refs, squares
        self.swap_sems, self.sems = sems
        me = lax.axis_index("dp")
        self.core, self.chip = lax.rem(me, 2), me // 2
        self.chips = n // 2
        self.right = lax.rem(self.chip + 1, self.chips)
        self.left = lax.rem(self.chip + self.chips - 1, self.chips)
        self.far = lax.rem(self.chip + 2, self.chips)
        self.row = (self.core * self.chips + self.chip) * got_near.shape[2]
        self.share = got_near.shape[2]

    def to(self, chip, core):
        return {"dp": chip * 2 + core}

    def barrier(self, far):
        barrier = pltpu.get_barrier_semaphore()
        peers = [(self.chip, 1 - self.core), (self.right, self.core), (self.left, self.core)]
        if far:
            peers.append((self.far, self.core))
            peers += [(chip, 1 - self.core) for chip in (self.right, self.left, self.far)]
        for peer in peers:
            pl.semaphore_signal(barrier, inc=1, device_id=self.to(*peer), device_id_type=MESH)
        pl.semaphore_wait(barrier, len(peers))

    def swap(self, u, slot):
        rows = self.share * self.chips
        other = pl.ds(pl.multiple_of((1 - self.core) * rows, rows), rows)
        return pltpu.make_async_remote_copy(
            src_ref=self.g_buf.at[slot, other],
            dst_ref=self.got_half.at[u],
            send_sem=self.swap_sems.at[0, u],
            recv_sem=self.swap_sems.at[1, u],
            device_id=self.to(self.chip, 1 - self.core),
            device_id_type=MESH,
        )

    def at(self, slot, chip, top=True, bottom=True):
        start = (self.core * self.chips + chip) * self.share + (0 if top else self.share // 2)
        size = self.share if top and bottom else self.share // 2
        return self.g_buf.at[slot, pl.ds(pl.multiple_of(start, size), size)]

    def copy(self, u, slot, which):
        top, bottom = pl.ds(0, self.share // 2), pl.ds(self.share // 2, self.share // 2)
        source, target, chip = {
            0: (self.at(slot, self.far, bottom=False), self.got_far.at[u, 0], self.right),
            1: (self.at(slot, self.far, top=False), self.got_far.at[u, 1], self.left),
            2: (self.at(slot, self.right, top=False), self.got_near.at[u, 0, bottom], self.right),
            3: (self.at(slot, self.left, bottom=False), self.got_near.at[u, 1, top], self.left),
            4: (self.at(slot, self.right, bottom=False), self.got_near.at[u, 0, top], self.right),
            5: (self.at(slot, self.left, top=False), self.got_near.at[u, 1, bottom], self.left),
        }[which]
        return pltpu.make_async_remote_copy(
            src_ref=source,
            dst_ref=target,
            send_sem=self.sems.at[0, u, which],
            recv_sem=self.sems.at[1, u, which],
            device_id=self.to(chip, self.core),
            device_id_type=MESH,
        )

    def first(self, u, slot):
        self.swap(u, slot).wait()
        for chip in range(self.chips):
            there = pl.ds(chip * self.share, self.share)
            mine = self.at(slot, chip)
            mine[...] = (mine[...].astype(F32) + self.got_half[u, there, :].astype(F32)).astype(BF16)
        for which in range(4):
            self.copy(u, slot, which).start()

    def second(self, u, slot):
        for which, mine in ((0, self.at(slot, self.right, bottom=False)), (1, self.at(slot, self.left, top=False))):
            self.copy(u, slot, which).wait_recv()
            mine[...] = (mine[...].astype(F32) + self.got_far[u, which].astype(F32)).astype(BF16)
            self.copy(u, slot, which + 4).start()

    def third(self, u, slot):
        for which in range(2, 6):
            self.copy(u, slot, which).wait_recv()
        total = self.at(slot, self.chip)[...].astype(F32) + self.got_near[u, 0].astype(F32) + self.got_near[u, 1].astype(F32)
        total = total.astype(BF16)
        if len(self.own_refs) == 1:
            self.own_refs[0][u] = total
        else:
            for part, half in zip(self.own_refs, (total[: self.share // 2], total[self.share // 2 :]), strict=True):
                part[u] = half
        wide = total.astype(F32)
        wide = (wide * wide).reshape(-1, 8, wide.shape[-1]).sum(0)
        self.squares[...] += sum(wide[:, i : i + 128] for i in range(0, wide.shape[-1], 128))
        for which in range(6):
            self.copy(u, slot, which).wait_send()


class Gather:
    def __init__(self, ex, own_ref, first, g_ref, sems, local_sem):
        self.ex, self.own_ref, self.first, self.g_ref, self.sems, self.local_sem = ex, own_ref, first, g_ref, sems, local_sem

    def rows(self, u, chip, top=True, bottom=True):
        ex = self.ex
        start = (ex.core * ex.chips + chip) * ex.share + (0 if top else ex.share // 2)
        size = ex.share if top and bottom else ex.share // 2
        return self.g_ref.at[u, pl.ds(pl.multiple_of(start, size), size)]

    def copy(self, u, which):
        ex = self.ex
        here = (ex.chip, 1 - ex.core)
        mine = self.rows(u, ex.chip)
        source, target, to = {
            0: (self.own_ref.at[self.first + u], mine, (ex.right, ex.core)),
            1: (self.own_ref.at[self.first + u], mine, (ex.left, ex.core)),
            2: (self.own_ref.at[self.first + u], mine, here),
            3: (self.rows(u, ex.left, bottom=False),) * 2 + ((ex.right, ex.core),),
            4: (self.rows(u, ex.right, top=False),) * 2 + ((ex.left, ex.core),),
            5: (self.rows(u, ex.left),) * 2 + (here,),
            6: (self.rows(u, ex.right),) * 2 + (here,),
            7: (self.rows(u, ex.far, bottom=False),) * 2 + (here,),
            8: (self.rows(u, ex.far, top=False),) * 2 + (here,),
        }[which]
        return pltpu.make_async_remote_copy(
            src_ref=source,
            dst_ref=target,
            send_sem=self.sems.at[0, u, which],
            recv_sem=self.sems.at[1, u, which],
            device_id=ex.to(*to),
            device_id_type=MESH,
        )

    def local(self, u):
        return pltpu.make_async_copy(self.own_ref.at[self.first + u], self.rows(u, self.ex.chip), self.local_sem.at[u])

    def one(self, u):
        for which in range(3):
            self.copy(u, which).start()
        self.local(u).start()

    def two(self, u):
        for which in range(2):
            self.copy(u, which).wait_recv()
            self.copy(u, which + 3).start()
            self.copy(u, which + 5).start()

    def three(self, u):
        for which in range(2):
            self.copy(u, which + 3).wait_recv()
            self.copy(u, which + 7).start()

    def four(self, u):
        for which in (2, 5, 6, 7, 8):
            self.copy(u, which).wait_recv()
        for which in range(9):
            self.copy(u, which).wait_send()
        self.local(u).wait()


def squares_over_group(ex, squares_ref, slots, sems):
    me = ex.chip * 2 + ex.core
    n = 2 * ex.chips

    def send(i):
        return pltpu.make_async_remote_copy(
            src_ref=squares_ref,
            dst_ref=slots.at[me],
            send_sem=sems.at[0, i],
            recv_sem=sems.at[1, i],
            device_id={"dp": lax.rem(me + i, n)},
            device_id_type=MESH,
        )

    copies = [send(i) for i in range(1, n)]
    for copy in copies:
        copy.start()
    slots[me] = squares_ref[...]
    for copy in copies:
        copy.wait()
    total = slots[0]
    for i in range(1, n):
        total = total + slots[i]
    squares_ref[...] = total


def backward_kernel(n, with_da, h_ref, dy_ref, *refs):
    if with_da:
        wg_ref, wu_ref, wd_ref, squares_ref, gathered_ref, own_ref, dh_ref, a_buf, acc, *refs = refs
        own_refs = (own_ref,)
    else:
        wd_ref, gate_hbm, up_hbm, earlier_own_ref, earlier_squares_ref, squares_ref, gathered_ref, *own_refs, stage, stage_sems = refs[:11]
        refs = refs[11:]
    t_buf, gu_buf, g_buf, got_half, got_far, got_near, slots, *sems = refs
    swap_sems, copy_sems, gather_sems, local_sems, slot_sems = sems
    depth = g_buf.shape[0]
    s = pl.program_id(0)
    last = pl.num_programs(0) - 1
    _, tokens, d = h_ref.shape
    steps = tokens // CHUNK
    ex = Exchange(n, g_buf, got_half, got_far, got_near, own_refs, squares_ref, (swap_sems, copy_sems))
    gather = Gather(ex, own_ref if with_da else earlier_own_ref, 0, gathered_ref, gather_sems, local_sems)

    def chunk(t):
        return pl.ds(pl.multiple_of(t * CHUNK, CHUNK), CHUNK)

    def each(f, start=0):
        lax.fori_loop(0, 3, lambda j, _: (f(start + j), 0)[1], 0)

    def fetch(step):
        slot = lax.rem(step, 2)
        return [pltpu.make_async_copy(kept.at[step // steps, chunk(lax.rem(step, steps))], stage.at[slot, i], stage_sems.at[slot, i]) for i, kept in enumerate((gate_hbm, up_hbm))]

    @pl.when(s == 0)
    def _():
        if not with_da:
            for copy in fetch(0):
                copy.start()
        ex.barrier(not with_da)
        if with_da:
            squares_ref[...] = jnp.zeros_like(squares_ref)
        else:
            squares_ref[...] = earlier_squares_ref[...]
            each(gather.one)

        def prepare(t, _):
            rows = chunk(t)
            a = normed(h_ref[0, rows, :])
            t_buf[0, :, rows] = a.T
            t_buf[1, :, rows] = dy_ref[0, rows, :].T
            if with_da:
                a_buf[rows, :] = a
                acc[rows, :] = jnp.zeros((CHUNK, d), F32)
            return 0

        lax.fori_loop(0, steps, prepare, 0)

    def due(u, what):
        steps = {"f": ex.first, "s": ex.second, "t": ex.third}
        gathers = {"1": gather.one, "2": gather.two, "3": gather.three, "4": gather.four}
        for step, j in zip(what[::2], map(int, what[1::2])):
            if step in steps:
                steps[step](u + j, lax.rem(u + j, depth))
            else:
                gathers[step](u + j)

    here, before = 3 * s, 3 * (s - 1)

    def when(condition, *actions):
        @pl.when(condition)
        def _():
            for action in actions:
                action()

    if with_da:
        in_hidden = {1: "s2", 2: "t010t111", 3: "t212"}
        in_weights = {0: "20", 1: "21", 2: "22"}
        in_da = {1: "f2", 2: "s0", 3: "s1"}
        before_in_da = {0: "30", 1: "31", 3: "32"}
        earlier_in_hidden = {0: "404142"}
    else:
        in_hidden = {1: "f2", 2: "s0"}
        in_weights = {0: "s1", 1: "s2", 2: "t0"}
        earlier_in_hidden = {0: "t1", 2: "t2"}

    def hidden(t, _):
        for i, what in in_hidden.items():
            when((s > 0) & (t == i), functools.partial(due, before, what))
        for i, what in earlier_in_hidden.items():
            when((s > 1) & (t == i), functools.partial(due, before - 3, what))
        if not with_da:
            when((s == 0) & (t == 3), functools.partial(due, 0, "20"))
            when((s == 1) & (t == 0), functools.partial(due, 0, "31"))
            when((s == 1) & (t == 2), functools.partial(due, 0, "32"))
        rows = chunk(t)
        if with_da:
            a = a_buf[rows, :]
            gate = dot(a, wg_ref[0])
            up = dot(a, wu_ref[0])
        else:
            step = s * steps + t
            for copy in fetch(step):
                copy.wait()
            when(step + 1 < pl.num_programs(0) * steps, lambda: [copy.start() for copy in fetch(step + 1)])
            gate, up = stage[lax.rem(step, 2), 0], stage[lax.rem(step, 2), 1]
        dact = dot_nt(dy_ref[0, rows, :], wd_ref[0]).astype(BF16).astype(F32)
        sig = jax.nn.sigmoid(gate)
        silu = gate * sig
        gu_buf[0, rows, :] = (dact * up * (sig + silu * (1 - sig))).astype(BF16)
        gu_buf[1, rows, :] = (dact * silu).astype(BF16)
        gu_buf[2, rows, :] = (silu * up).astype(BF16)
        return 0

    lax.fori_loop(0, steps, hidden, 0)

    def weights(j, _):
        for i, what in in_weights.items():
            when((s > 0) & (j == i), functools.partial(due, before, what))
        if not with_da:
            when((s == 0) & (j == 1), functools.partial(due, 0, "21"))
            when((s == 0) & (j == 2), functools.partial(due, 0, "2230"))
            when((s == 1) & (j == 0), functools.partial(due, 0, "404142"))
        slot = lax.rem(here + j, depth)
        g_buf[slot] = dot(t_buf[j // 2], gu_buf[j]).astype(BF16)
        ex.swap(here + j, slot).start()
        when(j > 0, lambda: ex.first(here + j - 1, lax.rem(here + j - 1, depth)))
        return 0

    lax.fori_loop(0, 3, weights, 0)

    if with_da:

        def by_a(t, _):
            for i, what in in_da.items():
                when(t == i, functools.partial(due, here, what))
            for i, what in before_in_da.items():
                when((s > 0) & (t == i), functools.partial(due, before, what))
            rows = chunk(t)
            acc[rows, :] += dot_nt(gu_buf[0, rows, :], wg_ref[0]) + dot_nt(gu_buf[1, rows, :], wu_ref[0])
            return 0

        lax.fori_loop(0, steps, by_a, 0)

    @pl.when(s == last)
    def _():
        if with_da:

            def by_h(t, _):
                rows = chunk(t)
                wide = h_ref[0, rows, :].astype(F32)
                scale = norm_scale(wide)
                da = acc[rows, :].astype(BF16).astype(F32)
                through = da * scale - wide * (scale * scale * scale * jnp.mean(da * wide, -1, keepdims=True))
                dh_ref[0, rows, :] = dy_ref[0, rows, :] + through.astype(BF16)
                return 0

            lax.fori_loop(0, steps // 2, by_h, 0)
            due(here, "s2t0")
            lax.fori_loop(steps // 2, steps, by_h, 0)
            due(before, "404142")
            due(here, "t1t2")
        else:
            due(here, "s0f2")
            due(before, "t1t2")
            due(here, "s1t0s2t1t2")
            squares_over_group(ex, squares_ref, slots, slot_sems)


def backward(n, layer, with_da, h, dy, weights, earlier=()):
    _, tokens, d = h.shape
    ff = weights[0].shape[-1]
    units = 3 * (ff // WIDTH)
    share, chips = d // n, n // 2
    gathered = units - 3 if with_da else 3
    out_shape = [
        jax.ShapeDtypeStruct((8, 128), F32),
        jax.ShapeDtypeStruct((gathered, d, WIDTH), BF16),
    ]
    out_specs = [once(out_shape[0].shape), pl.BlockSpec(memory_space=pl.ANY)]
    if with_da:
        out_shape += [jax.ShapeDtypeStruct((units, share, WIDTH), BF16), jax.ShapeDtypeStruct(h.shape, BF16)]
        more = weight_specs(layer, d)
        scratch = [pltpu.VMEM((tokens, d), BF16), pltpu.VMEM((tokens, d), F32)]
    else:
        out_shape += [jax.ShapeDtypeStruct((units, share // 2, WIDTH), BF16)] * 2
        last = units // 3 - 1
        anywhere = pl.BlockSpec(memory_space=pl.ANY)
        share_spec = pl.BlockSpec((3, share, WIDTH), lambda s: (last, 0, 0), pipeline_mode=pl.Buffered(1))
        more = weight_specs(layer, d)[2:] + [anywhere, anywhere, share_spec, once((8, 128))]
        weights = weights[2:]
        scratch = [pltpu.VMEM((2, 2, CHUNK, WIDTH), F32), pltpu.SemaphoreType.DMA((2, 2))]
    out_specs += [once(o.shape) for o in out_shape[2:]]
    return pl.pallas_call(
        functools.partial(backward_kernel, n, with_da),
        grid=(ff // WIDTH,),
        in_specs=[once(h.shape), once(h.shape)] + more,
        out_specs=out_specs,
        out_shape=out_shape,
        scratch_shapes=scratch
        + [
            pltpu.VMEM((2, d, tokens), BF16),
            pltpu.VMEM((3, tokens, WIDTH), BF16),
            pltpu.VMEM((SLOTS, d, WIDTH), BF16),
            pltpu.VMEM((units, chips * share, WIDTH), BF16),
            pltpu.VMEM((units, 2, share // 2, WIDTH), BF16),
            pltpu.VMEM((units, 2, share, WIDTH), BF16),
            pltpu.VMEM((n, 8, 128), F32),
            pltpu.SemaphoreType.DMA((2, units)),
            pltpu.SemaphoreType.DMA((2, units, 6)),
            pltpu.SemaphoreType.DMA((2, gathered, 9)),
            pltpu.SemaphoreType.DMA((gathered,)),
            pltpu.SemaphoreType.DMA((2, n)),
        ],
        compiler_params=pltpu.CompilerParams(
            vmem_limit_bytes=VMEM_LIMIT, dimension_semantics=("arbitrary",), collective_id=1 + layer, has_side_effects=True
        ),
        name=f"backward_{layer}",
    )(h, dy, *weights, *earlier)


def adamw_kernel(count, rows_ref, q_ref, pieces, refs):
    ws, ms, vs = refs[0:3], refs[3:6], refs[6:9]
    new_ws, new_ms, new_vs = refs[9:12], refs[12:15], refs[15:18]
    factor = jnp.minimum(1.0, 0.5 * lax.rsqrt(jnp.full((1, 1), jnp.sum(q_ref[...]) / count, F32) + 1e-30))

    def update(g, w, m, v, new_w, new_m, new_v, rows, columns):
        at = (0, rows, columns)
        g = g * factor
        m = 0.9 * m[at] + 0.1 * g
        v = 0.95 * v[at] + 0.05 * g * g
        new_m[at] = m
        new_v[at] = v
        wide = w[at].astype(F32)
        new_w[at] = (wide - 0.02 * (m * lax.rsqrt(v + 1e-8) + 0.1 * wide)).astype(BF16)

    everything = list(zip(ws, ms, vs, new_ws, new_ms, new_vs, strict=True))
    g_ref = pieces[0]
    if len(pieces) > 1:
        g_ref = refs[18]
        for i, piece in enumerate(pieces):
            size = piece.shape[1]
            for j in range(3):
                g_ref[j, pl.ds(pl.multiple_of(rows_ref[i], size), size), :] = piece[j]
    d = g_ref.shape[1]
    for j in range(2):
        for row in range(0, d, 192):
            rows = slice(row, row + 192)
            update(g_ref[j, rows, :].astype(F32), *everything[j], rows, slice(None))
    for row in range(0, d, 384):
        rows = slice(row, row + 384)
        update(g_ref[2, rows, :].astype(F32).T, *everything[2], slice(None), rows)


def adamw(squares, layer, slices, pieces, rows, weights, m, v, earlier):
    layers, d, ff = weights[0].shape
    strips = WIDTH // STRIP
    start = slices[0] * strips
    wide = pl.BlockSpec((1, d, STRIP), lambda s: (layer, 0, start + s))
    tall = pl.BlockSpec((1, STRIP, d), lambda s: (layer, start + s, 0))
    three = [wide, wide, tall]
    anywhere = [pl.BlockSpec(memory_space=pl.ANY)] * len(earlier)
    count = sum(w.size for w in weights)
    k, parts = len(pieces), slices[1] - slices[0]

    def kernel(rows_ref, q_ref, *refs):
        refs = refs[: k + 9] + refs[k + 9 + len(earlier) :]
        adamw_kernel(count, rows_ref, q_ref, refs[:k], refs[k:])

    return pl.pallas_call(
        kernel,
        grid=(parts * strips,),
        in_specs=[pl.BlockSpec(memory_space=pltpu.SMEM), once((8, 128))]
        + [pl.BlockSpec((3, g.shape[1], STRIP), lambda s: (s // strips, 0, s % strips)) for g in pieces]
        + three * 3
        + anywhere,
        out_specs=three * 3,
        out_shape=[jax.ShapeDtypeStruct(w.shape, t) for t in (BF16, F32, F32) for w in weights],
        scratch_shapes=[pltpu.VMEM((3, d, STRIP), BF16)] if k > 1 else [],
        input_output_aliases={11 + k + i: i for i in range(len(earlier))},
        compiler_params=pltpu.CompilerParams(vmem_limit_bytes=VMEM_LIMIT, dimension_semantics=("arbitrary",)),
        cost_estimate=pl.CostEstimate(flops=10**11 // 6 * parts, bytes_accessed=39 * 10**6 * parts, transcendentals=0),
        name=f"adamw_{layer}_{slices[0]}",
    )(rows, squares, *pieces, *weights, *m, *v, *earlier)


def gathered(n, own, first, second):
    chips, half = n // 2, own[0].shape[1]
    share = 2 * half
    me = lax.axis_index("dp")
    core, chip = me % 2, me // 2
    left, right, far = (chip + chips - 1) % chips, (chip + 1) % chips, (chip + 2) % chips

    def shift(a, by):
        return lax.ppermute(a, "dp", [(c * 2 + k, (c + by) % chips * 2 + k) for c in range(chips) for k in range(2)])

    def swap(a):
        return lax.ppermute(a, "dp", [(i, i ^ 1) for i in range(n)])

    top, bottom = own
    from_left = [shift(top, 1), shift(bottom, 1)]
    from_right = [shift(bottom, -1), shift(top, -1)]
    result = first()
    from_left, from_right, result = lax.optimization_barrier((from_left, from_right, result))
    far_top, far_bottom = shift(from_left[0], 1), shift(from_right[0], -1)
    near = [top, bottom, *from_left, *from_right]
    near_there = [swap(piece) for piece in near]
    result = second(result)
    far_top, far_bottom, result = lax.optimization_barrier((far_top, far_bottom, result))
    pieces = near + [far_top, far_bottom] + near_there + [swap(far_top), swap(far_bottom)]
    rows = [chip * share, chip * share + half, left * share, left * share + half, right * share + half, right * share, far * share, far * share + half]
    rows = [core * chips * share + row for row in rows] + [(1 - core) * chips * share + row for row in rows]
    return pieces, jnp.stack(rows).astype(jnp.int32), result


def solution(mesh):
    n = mesh.shape["dp"]

    def step(x, dy, *arrays):
        weights, m, v = (arrays[i : i + 3] for i in (0, 3, 6))
        slices = weights[0].shape[-1] // WIDTH
        h, gate, up = forward(0, x, weights)
        squares, g_1, own_1, dh = backward(n, 1, True, h, dy, weights)
        squares, g_1_last, *own_0 = backward(n, 0, False, x, dh, weights, (gate, up, own_1, squares))
        nowhere = jnp.zeros((1,), jnp.int32)
        pieces, rows, new = gathered(
            n,
            own_0,
            lambda: adamw(squares, 1, (0, slices - 1), [g_1], nowhere, weights, m, v, ()),
            lambda new: adamw(squares, 1, (slices - 1, slices), [g_1_last], nowhere, weights, m, v, new),
        )
        return tuple(adamw(squares, 0, (0, slices), pieces, rows, weights, m, v, new))

    return jax.shard_map(
        step,
        mesh=mesh,
        in_specs=(P(("rep", "dp"), None, None),) * 2 + (P(None, None, None),) * 9,
        out_specs=(P("rep", None, None),) * 9,
        check_vma=False,
    )
```
